16 devices in a mesh: rep: 4 (over y, z, core), dp: 4 (over x).
Axes of the slice: x: 4, y: 2, z: 1, core: 2. Of those that a mesh axis runs over, the one named last changes fastest.
The devices are a block of a 4x4x8 slice.
Arguments:
- x: bfloat16 [16, 4096, 1024], P(('rep', 'dp')), parts along dimension 0
- dy: bfloat16 [16, 4096, 1024], P(('rep', 'dp')), parts along dimension 0
- w_gate: bfloat16 [2, 1024, 2816], replicated
- w_up: bfloat16 [2, 1024, 2816], replicated
- w_down: bfloat16 [2, 2816, 1024], replicated
- m_w_gate: float32 [2, 1024, 2816], P(None, 'dp')
- m_w_up: float32 [2, 1024, 2816], P(None, 'dp')
- m_w_down: float32 [2, 2816, 1024], P(None, 'dp')
- v_w_gate: float32 [2, 1024, 2816], P(None, 'dp')
- v_w_up: float32 [2, 1024, 2816], P(None, 'dp')
- v_w_down: float32 [2, 2816, 1024], P(None, 'dp')
Outputs:
- output 1: bfloat16 [8, 1024, 2816], P('rep'), parts along dimension 0
- output 2: bfloat16 [8, 1024, 2816], P('rep'), parts along dimension 0
- output 3: bfloat16 [8, 2816, 1024], P('rep'), parts along dimension 0
- output 4: float32 [8, 1024, 2816], P('rep', 'dp'), parts along dimension 0
- output 5: float32 [8, 1024, 2816], P('rep', 'dp'), parts along dimension 0
- output 6: float32 [8, 2816, 1024], P('rep', 'dp'), parts along dimension 0
- output 7: float32 [8, 1024, 2816], P('rep', 'dp'), parts along dimension 0
- output 8: float32 [8, 1024, 2816], P('rep', 'dp'), parts along dimension 0
- output 9: float32 [8, 2816, 1024], P('rep', 'dp'), parts along dimension 0
There are 4 independent parts. The reference program is written for one: setup_inputs(seed, part) draws one part's arguments, and reference() takes and returns one part's arrays. A program takes and returns all parts, laid end to end along the dimension named above; an argument that names none is the same for every part.
All inputs are finite; a program needn't handle non-finite values.
Results may differ from the reference program's by a relative error of at most 0.022.
Values are sent between devices in bfloat16 or wider.
A program may use at most 768 MiB of HBM per device.

```python
import jax
import jax.numpy as jnp
from jax import lax

SEQUENCES = 4
TOKENS = 4096
D = 1024
FF = 2816
LAYERS = 2
NAMES = ("w_gate", "w_up", "w_down")
SHAPES = {"w_gate": (LAYERS, D, FF), "w_up": (LAYERS, D, FF), "w_down": (LAYERS, FF, D)}


def bump(key, n, height):
    away = (jnp.arange(n, dtype=jnp.int32) - jax.random.randint(key, (), 0, n, jnp.int32)) % n
    return jnp.where(away < n // 8, height, 1.0)


def together(key, own, strength):
    shared = jax.random.normal(key, own.shape[1:], jnp.float32)
    return (own + strength * shared) * lax.rsqrt(1 + strength * strength)


def setup_inputs(seed: int = 0, part: int = 0) -> dict:
    kx, kdy, ka, kb, kz, kf, kh, kl, *keys = jax.random.split(jax.random.key(seed), 8 + 3 * len(NAMES))
    kx, kdy, ka, kb = (jax.random.fold_in(k, part) for k in (kx, kdy, ka, kb))
    kw, km, kv = (keys[i::3] for i in range(3))
    shape = (SEQUENCES, TOKENS, D)
    much_x, much_dy = jax.random.uniform(kz, (2,), jnp.float32, 0.0, 1.0)
    loud = 2.0 ** jax.random.uniform(jax.random.fold_in(kz, 1), (), jnp.float32, -1.0, 2.0)
    layers = 2.0 ** jax.random.uniform(kl, (LAYERS, 1, 1), jnp.float32, -1.0, 1.0)
    x = together(ka, jax.random.normal(kx, shape, jnp.float32), much_x) * bump(kf, D, 4.0)
    dy = together(kb, jax.random.normal(kdy, shape, jnp.float32), much_dy)
    drawn = {"x": x.astype(jnp.bfloat16), "dy": (loud * dy * (SEQUENCES * TOKENS) ** -0.5).astype(jnp.bfloat16)}
    for key, name in zip(kw, NAMES, strict=True):
        w = jax.random.normal(key, SHAPES[name], jnp.float32) * SHAPES[name][1] ** -0.5
        drawn[name] = (w * {"w_gate": 1.0, "w_up": bump(kh, FF, 4.0), "w_down": layers}[name]).astype(jnp.bfloat16)
    for key, name in zip(km, NAMES, strict=True):
        drawn[f"m_{name}"] = 0.1 * jax.random.normal(key, SHAPES[name], jnp.float32)
    for key, name in zip(kv, NAMES, strict=True):
        drawn[f"v_{name}"] = jax.random.uniform(key, SHAPES[name], jnp.float32, 0.005, 0.015)
    return drawn


def matmul(a, w):
    return jnp.dot(a, w, preferred_element_type=jnp.float32).astype(jnp.bfloat16)


def normed(h):
    wide = h.astype(jnp.float32)
    scale = lax.rsqrt(jnp.mean(wide**2, -1, keepdims=True) + 1e-6)
    return (wide * scale).astype(jnp.bfloat16)


def layer(h, w):
    a = normed(h)
    gate = jnp.dot(a, w["w_gate"], preferred_element_type=jnp.float32)
    up = jnp.dot(a, w["w_up"], preferred_element_type=jnp.float32)
    return h + matmul((jax.nn.silu(gate) * up).astype(jnp.bfloat16), w["w_down"])


def adamw(w, m, v, g):
    m = 0.9 * m + 0.1 * g
    v = 0.95 * v + 0.05 * g * g
    step = m * lax.rsqrt(v + 1e-8) + 0.1 * w
    return (w - 0.02 * step).astype(jnp.bfloat16), m, v


def clipped(gradients, sum_of_squares, count):
    factor = jnp.minimum(1.0, 0.5 * lax.rsqrt(sum_of_squares / count + 1e-30))
    return [g * factor for g in gradients]


def stack(weights, h):
    return lax.scan(lambda h, w: (layer(h, w), None), h, weights)[0]


def reference(x, dy, w_gate, w_up, w_down, m_w_gate, m_w_up, m_w_down, v_w_gate, v_w_up, v_w_down):
    weights = dict(zip(NAMES, (w_gate, w_up, w_down), strict=True))

    def take(so_far, sequence):
        h, by_y = sequence
        _, back = jax.vjp(lambda w: stack(w, h), weights)
        return jax.tree.map(lambda total, term: total + term.astype(jnp.float32), so_far, back(by_y)[0]), None

    none_yet = {name: jnp.zeros(w.shape, jnp.float32) for name, w in weights.items()}
    by_weights, _ = lax.scan(take, none_yet, (x, dy))
    gradients = [by_weights[name].astype(jnp.bfloat16).astype(jnp.float32) for name in NAMES]
    gradients = clipped(gradients, sum(jnp.sum(g * g) for g in gradients), sum(g.size for g in gradients))
    new = [
        adamw(w.astype(jnp.float32), m, v, g)
        for w, m, v, g in zip((w_gate, w_up, w_down), (m_w_gate, m_w_up, m_w_down), (v_w_gate, v_w_up, v_w_down), gradients, strict=True)
    ]
    return tuple(one[which] for which in range(3) for one in new)
```

```python
import functools

import jax
import jax.numpy as jnp
from jax import lax
from jax.experimental import pallas as pl
from jax.experimental.pallas import tpu as pltpu
from jax.sharding import PartitionSpec as P

BF = jnp.bfloat16
F32 = jnp.float32
VMEM_LIMIT = 67_000_000
MESH = pl.DeviceIdType.MESH
NN = (((1,), (0,)), ((), ()))
NT = (((1,), (1,)), ((), ()))
ONE = pl.Buffered(1)
STEPS = 11
TILE = 512


def dot(a, b, dims):
    return lax.dot_general(a, b, dims, preferred_element_type=F32)


def first_strip(c):
    return jnp.where(c == 10, 5, jnp.where(c % 2 == 0, c // 2, 11 + c // 2))


def second_strip(c):
    return jnp.where(c == 10, 16, jnp.where(c % 2 == 0, 6 + c // 2, 17 + c // 2))


def normed(wide):
    scale = lax.rsqrt(jnp.mean(wide * wide, -1, keepdims=True) + 1e-6)
    return (wide * scale).astype(BF), scale


def forward_kernel(x_ref, dy_ref, wg_ref, wu_ref, wd_ref, gate_ref, up_ref, at0_ref, h_ref, a1_ref, at1_ref, dyt_ref, act):
    dyt_ref[...] = dy_ref[...].T
    sub = TILE // 2
    for i in range(2):
        rows = slice(i * sub, (i + 1) * sub)
        a, _ = normed(x_ref[rows, :].astype(F32))
        at0_ref[:, rows] = a.T
        for c in range(STEPS):
            cols = slice(256 * c, 256 * (c + 1))
            gate = dot(a, wg_ref[:, cols], NN)
            up = dot(a, wu_ref[:, cols], NN)
            gate_ref[rows, cols] = gate
            up_ref[rows, cols] = up
            act[rows, cols] = (gate * jax.nn.sigmoid(gate) * up).astype(BF)
    for i in range(2):
        rows = slice(i * sub, (i + 1) * sub)
        down = dot(act[rows, :], wd_ref[...], NN).astype(BF)
        h = (x_ref[rows, :].astype(F32) + down.astype(F32)).astype(BF)
        h_ref[rows, :] = h
        a1, _ = normed(h.astype(F32))
        a1_ref[rows, :] = a1
        at1_ref[:, rows] = a1.T


def forward(x, dy, wg, wu, wd):
    tokens, d = x.shape
    ff = wg.shape[2]
    row = pl.BlockSpec((TILE, d), lambda i: (i, 0))
    col = pl.BlockSpec((d, TILE), lambda i: (0, i))
    wide = pl.BlockSpec((TILE, ff), lambda i: (i, 0))
    up_spec = pl.BlockSpec((None, d, ff), lambda i: (0, 0, 0), pipeline_mode=ONE)
    down_spec = pl.BlockSpec((None, ff, d), lambda i: (0, 0, 0), pipeline_mode=ONE)
    s = jax.ShapeDtypeStruct
    return pl.pallas_call(
        forward_kernel,
        grid=(tokens // TILE,),
        in_specs=[row, row, up_spec, up_spec, down_spec],
        out_specs=[wide, wide, col, row, row, col, col],
        out_shape=[s((tokens, ff), F32), s((tokens, ff), F32), s((d, tokens), BF), s((tokens, d), BF), s((tokens, d), BF), s((d, tokens), BF), s((d, tokens), BF)],
        scratch_shapes=[pltpu.VMEM((TILE, ff), BF)],
        compiler_params=pltpu.CompilerParams(vmem_limit_bytes=VMEM_LIMIT),
        name="fwd0",
    )(x, dy, wg, wu, wd)


class Ring:
    def __init__(self, item, rows, refs, emit):
        self.item = item
        self.rows = rows
        self.term, self.recv, self.send, self.fin, self.ssem, self.rsem, self.fsem, self.total = refs
        self.emit = emit

    def copy(self, h, d, k, half):
        me = lax.axis_index("dp")
        to = lax.rem(me + (1 if d == 0 else 3), 4)
        slot = lax.rem(k, 2)
        if h == 0:
            src = self.term.at[lax.rem(k, self.term.shape[0]), pl.ds(self.start(h, d, half, True), half), :]
        else:
            src = self.send.at[h - 1, d, slot, pl.ds(0, half), :]
        return pltpu.make_async_remote_copy(
            src_ref=src,
            dst_ref=self.recv.at[h, d, slot, pl.ds(0, half), :],
            send_sem=self.ssem.at[h, d, slot],
            recv_sem=self.rsem.at[h, d, slot],
            device_id={"dp": to},
            device_id_type=MESH,
        )

    def start(self, h, d, half, sending):
        me = lax.axis_index("dp")
        away = h + 1 if sending else h + 2
        block = lax.rem(me + 8 - away, 4) if d == 0 else lax.rem(me + away, 4)
        return pl.multiple_of(block * 2 * half + d * half, half)

    def each(self, t, body):
        there, k = self.item(t)
        for condition, half in self.rows:
            where = there if condition is None else jnp.logical_and(there, condition(k))
            pl.when(where)(functools.partial(body, k, half))

    def point(self, t):
        def arrived(h, k, half):
            for d in range(2):
                self.copy(h, d, k, half).wait()

        def add(h, k, half):
            slot = lax.rem(k, 2)
            for d in range(2):
                mine = self.term[lax.rem(k, self.term.shape[0]), pl.ds(self.start(h, d, half, False), half), :]
                value = (self.recv[h, d, slot, pl.ds(0, half), :].astype(F32) + mine.astype(F32)).astype(BF)
                if h < 2:
                    self.send[h, d, slot, pl.ds(0, half), :] = value
                else:
                    self.fin[slot, pl.ds(d * half, half), :] = value
                    wide = value.astype(F32)
                    square = wide * wide
                    parts = [square[:, 128 * i : 128 * (i + 1)] for i in range(square.shape[1] // 128)]
                    part = functools.reduce(jnp.add, parts)
                    self.total[...] += jnp.sum(part.reshape(half // 8, 8, 128), 0)

        def leave(h, k, half):
            for d in range(2):
                self.copy(h, d, k, half).start()

        def out(k, half):
            for c in self.emit(k, lax.rem(k, 2), 2 * half):
                c.start()

        def gone(k, half):
            for c in self.emit(k, lax.rem(k, 2), 2 * half):
                c.wait()

        for h in range(3):
            self.each(t - 1 - h, functools.partial(arrived, h))
        self.each(t - 4, gone)
        for h in range(3):
            self.each(t - 1 - h, functools.partial(add, h))
        for h in range(3):
            self.each(t - h, functools.partial(leave, h))
        self.each(t - 3, out)


def rings(c_refs, g_out, u_out, d_out):
    (g_term, u_term, d_term, g_recv, u_recv, d_recv, g_send, u_send, d_send, g_fin, u_fin, d_fin, ssem, rsem, fsem, total) = c_refs
    me = lax.axis_index("dp")

    def every(t):
        return jnp.logical_and(t >= 0, t < STEPS), t

    def pairs(t):
        last = t == 11
        return jnp.logical_or(last, jnp.logical_and(jnp.logical_and(t >= 2, t <= 10), lax.rem(t, 2) == 0)), jnp.where(last, 5, lax.div(t - 2, 2))

    def strips(fin, out, sem):
        def emit(k, slot, rows):
            return [
                pltpu.make_async_copy(
                    fin.at[slot, :, pl.ds(128 * i, 128)], out.at[:, pl.ds(pl.multiple_of(128 * strip(k), 128), 128)], sem.at[slot, i]
                )
                for i, strip in enumerate((first_strip, second_strip))
            ]

        return emit

    def down(k, slot, rows):
        odd = lax.rem(me, 2)
        at = 128 * k + 64 * odd if rows == 128 else 640 * (1 - odd)
        return [pltpu.make_async_copy(d_fin.at[slot, pl.ds(0, rows), :], d_out.at[pl.ds(pl.multiple_of(at, 64), rows), :], fsem.at[2, slot, 0])]

    g = Ring(every, [(None, 128)], (g_term, g_recv, g_send, g_fin, ssem.at[0], rsem.at[0], None, total), strips(g_fin, g_out, fsem.at[0]))
    u = Ring(every, [(None, 128)], (u_term, u_recv, u_send, u_fin, ssem.at[1], rsem.at[1], None, total), strips(u_fin, u_out, fsem.at[1]))
    d = Ring(
        pairs, [(lambda k: k < 5, 64), (lambda k: k == 5, 32)], (d_term, d_recv, d_send, d_fin, ssem.at[2], rsem.at[2], None, total), down
    )
    return g, u, d


def ring_scratch(d):
    v = pltpu.VMEM
    return [
        v((4, d, 256), BF),
        v((4, d, 256), BF),
        v((3, 512, d), BF),
        v((3, 2, 2, 128, 256), BF),
        v((3, 2, 2, 128, 256), BF),
        v((3, 2, 2, 64, d), BF),
        v((2, 2, 2, 128, 256), BF),
        v((2, 2, 2, 128, 256), BF),
        v((2, 2, 2, 64, d), BF),
        v((2, 256, 256), BF),
        v((2, 256, 256), BF),
        v((2, 128, d), BF),
        pltpu.SemaphoreType.DMA((3, 3, 2, 2)),
        pltpu.SemaphoreType.DMA((3, 3, 2, 2)),
        pltpu.SemaphoreType.DMA((3, 2, 2)),
        v((8, 128), F32),
    ]


def greet():
    me = lax.axis_index("dp")
    barrier = pltpu.get_barrier_semaphore()
    for other in (lax.rem(me + 1, 4), lax.rem(me + 3, 4)):
        pl.semaphore_signal(barrier, inc=1, device_id={"dp": other}, device_id_type=MESH)
    pl.semaphore_wait(barrier, 2)


def weight_gradients(c, at_ref, dyt_ref, dg, du, act, c_refs, g, u, d):
    g_term, u_term, d_term = c_refs[:3]
    g_term[lax.rem(c, 4)] = dot(at_ref[...], dg[...], NN).astype(BF)
    u_term[lax.rem(c, 4)] = dot(at_ref[...], du[...], NN).astype(BF)
    g.point(c)
    down = dot(dyt_ref[...], act[...], NN).astype(BF).T
    half = c // 2
    d_term[lax.rem(half, 3), pl.ds(pl.multiple_of(256 * lax.rem(c, 2), 256), 256), :] = down
    u.point(c)


def drain(c, c_refs, g, u, d, sq_ref):
    @pl.when(c == STEPS - 1)
    def _():
        def one(t, _):
            d.point(t)
            g.point(t)
            u.point(t)
            return 0

        lax.fori_loop(STEPS, STEPS + 5, one, 0)
        sq_ref[...] = c_refs[-1][...]


def layer1_kernel(a_ref, at_ref, dy_ref, dyt_ref, wg1, wg2, wu1, wu2, wd1, wd2, dgate_out, dup_out, g_out, u_out, d_out, sq_ref, act, dg, du, wg, wu, wd, osem, *c_refs):
    c = pl.program_id(0)
    g, u, d = rings(c_refs, g_out, u_out, d_out)

    def put(k):
        cols = pl.ds(pl.multiple_of(256 * k, 256), 256)
        return [pltpu.make_async_copy(dg, dgate_out.at[:, cols], osem.at[0]), pltpu.make_async_copy(du, dup_out.at[:, cols], osem.at[1])]

    @pl.when(c == 0)
    def _():
        greet()
        c_refs[-1][...] = jnp.zeros((8, 128), F32)

    wg[:, :128] = wg1[...]
    wg[:, 128:] = wg2[...]
    wu[:, :128] = wu1[...]
    wu[:, 128:] = wu2[...]
    wd[:128, :] = wd1[...]
    wd[128:, :] = wd2[...]

    @pl.when(c > 0)
    def _():
        for p in put(c - 1):
            p.wait()

    for i in range(a_ref.shape[0] // TILE):
        rows = slice(i * TILE, (i + 1) * TILE)
        gate = dot(a_ref[rows, :], wg[...], NN)
        up = dot(a_ref[rows, :], wu[...], NN)
        dact = dot(dy_ref[rows, :], wd[...], NT).astype(BF).astype(F32)
        s = jax.nn.sigmoid(gate)
        silu = gate * s
        act[rows, :] = (silu * up).astype(BF)
        du[rows, :] = (dact * silu).astype(BF)
        dg[rows, :] = (dact * up * (s + silu * (1.0 - s))).astype(BF)
    d.point(c)
    for p in put(c):
        p.start()
    weight_gradients(c, at_ref, dyt_ref, dg, du, act, c_refs, g, u, d)
    drain(c, c_refs, g, u, d, sq_ref)

    @pl.when(c == STEPS - 1)
    def _():
        for p in put(c):
            p.wait()


def layer1(a1, at1, dy, dyt, wg, wu, wd):
    tokens, d = a1.shape
    ff = wg.shape[2]
    s = jax.ShapeDtypeStruct
    whole = lambda shape: pl.BlockSpec(shape, lambda c: (0, 0), pipeline_mode=ONE)
    cols = lambda strip: pl.BlockSpec((None, d, 128), lambda c: (1, 0, strip(c)))
    rows = lambda strip: pl.BlockSpec((None, 128, d), lambda c: (1, strip(c), 0))
    anywhere = pl.BlockSpec(memory_space=pl.ANY)
    return pl.pallas_call(
        layer1_kernel,
        grid=(STEPS,),
        in_specs=[whole((tokens, d)), whole((d, tokens)), whole((tokens, d)), whole((d, tokens))]
        + [cols(first_strip), cols(second_strip)] * 2
        + [rows(first_strip), rows(second_strip)],
        out_specs=[anywhere] * 5 + [pl.BlockSpec((8, 128), lambda c: (0, 0))],
        out_shape=[s((tokens, ff), BF)] * 2 + [s((d // 4, ff), BF)] * 2 + [s((ff // 4, d), BF), s((8, 128), F32)],
        scratch_shapes=[pltpu.VMEM((tokens, 256), BF)] * 3
        + [pltpu.VMEM((d, 256), BF)] * 2
        + [pltpu.VMEM((256, d), BF), pltpu.SemaphoreType.DMA((2,))]
        + ring_scratch(d),
        compiler_params=pltpu.CompilerParams(vmem_limit_bytes=VMEM_LIMIT, collective_id=1, has_side_effects=True),
        name="layer1",
    )(a1, at1, dy, dyt, wg, wg, wu, wu, wd, wd)


def input_kernel(dg_ref, du_ref, h_ref, dy_ref, wg_any, wu_any, dh_ref, dht_ref, wg, wu, sem):
    def fetch():
        copies = []
        for which, (src, dst) in enumerate(((wg_any, wg), (wu_any, wu))):
            for c in range(STEPS):
                strips = (5, 16) if c == 10 else ((c // 2, 6 + c // 2) if c % 2 == 0 else (11 + c // 2, 17 + c // 2))
                for i, strip in enumerate(strips):
                    copies.append(
                        pltpu.make_async_copy(
                            src.at[1, :, pl.ds(128 * strip, 128)], dst.at[:, pl.ds(256 * c + 128 * i, 128)], sem.at[which, 2 * c + i]
                        )
                    )
        return copies

    @pl.when(pl.program_id(0) == 0)
    def _():
        copies = fetch()
        for c in copies:
            c.start()
        for c in copies:
            c.wait()

    sub = TILE // 2
    for i in range(2):
        rows = slice(i * sub, (i + 1) * sub)
        da = dot(dg_ref[rows, :], wg[...], NT).astype(BF).astype(F32) + dot(du_ref[rows, :], wu[...], NT).astype(BF).astype(F32)
        da = da.astype(BF).astype(F32)
        wide = h_ref[rows, :].astype(F32)
        scale = lax.rsqrt(jnp.mean(wide * wide, -1, keepdims=True) + 1e-6)
        along = jnp.sum(da * wide, -1, keepdims=True) * (scale * scale * scale) * (1.0 / wide.shape[-1])
        back = (da * scale - wide * along).astype(BF)
        dh = (dy_ref[rows, :].astype(F32) + back.astype(F32)).astype(BF)
        dh_ref[rows, :] = dh
        dht_ref[:, rows] = dh.T


def input_gradient(dg, du, h, dy, wg, wu):
    tokens, d = h.shape
    ff = dg.shape[1]
    row = pl.BlockSpec((TILE, d), lambda i: (i, 0))
    wide = pl.BlockSpec((TILE, ff), lambda i: (i, 0))
    anywhere = pl.BlockSpec(memory_space=pl.ANY)
    s = jax.ShapeDtypeStruct
    return pl.pallas_call(
        input_kernel,
        grid=(tokens // TILE,),
        in_specs=[wide, wide, row, row, anywhere, anywhere],
        out_specs=[row, pl.BlockSpec((d, TILE), lambda i: (0, i))],
        out_shape=[s((tokens, d), BF), s((d, tokens), BF)],
        scratch_shapes=[pltpu.VMEM((d, ff), BF)] * 2 + [pltpu.SemaphoreType.DMA((2, 22))],
        compiler_params=pltpu.CompilerParams(vmem_limit_bytes=VMEM_LIMIT),
        name="input1",
    )(dg, du, h, dy, wg, wu)


def layer0_kernel(dh_ref, dht_ref, at_ref, g1, g2, u1, u2, wd1, wd2, g_out, u_out, d_out, sq_ref, act, dg, du, wd, *c_refs):
    c = pl.program_id(0)
    g, u, d = rings(c_refs, g_out, u_out, d_out)

    @pl.when(c == 0)
    def _():
        greet()
        c_refs[-1][...] = jnp.zeros((8, 128), F32)

    wd[:128, :] = wd1[...]
    wd[128:, :] = wd2[...]
    for i in range(dh_ref.shape[0] // TILE):
        rows = slice(i * TILE, (i + 1) * TILE)
        dact_all = dot(dh_ref[rows, :], wd[...], NT).astype(BF).astype(F32)
        for j, (gate_ref, up_ref) in enumerate(((g1, u1), (g2, u2))):
            cols = slice(128 * j, 128 * (j + 1))
            dact, gate, up = dact_all[:, cols], gate_ref[rows, :], up_ref[rows, :]
            s = jax.nn.sigmoid(gate)
            silu = gate * s
            act[rows, cols] = (silu * up).astype(BF)
            du[rows, cols] = (dact * silu).astype(BF)
            dg[rows, cols] = (dact * up * (s + silu * (1.0 - s))).astype(BF)
    d.point(c)
    weight_gradients(c, at_ref, dht_ref, dg, du, act, c_refs, g, u, d)
    drain(c, c_refs, g, u, d, sq_ref)


def layer0(dh, dht, at0, gate, up, wd):
    tokens, d = dh.shape
    ff = gate.shape[1]
    s = jax.ShapeDtypeStruct
    whole = lambda shape: pl.BlockSpec(shape, lambda c: (0, 0), pipeline_mode=ONE)
    wide = lambda strip: pl.BlockSpec((tokens, 128), lambda c: (0, strip(c)))
    rows = lambda strip: pl.BlockSpec((None, 128, d), lambda c: (0, strip(c), 0))
    anywhere = pl.BlockSpec(memory_space=pl.ANY)
    return pl.pallas_call(
        layer0_kernel,
        grid=(STEPS,),
        in_specs=[whole((tokens, d)), whole((d, tokens)), whole((d, tokens))]
        + [wide(first_strip), wide(second_strip)] * 2
        + [rows(first_strip), rows(second_strip)],
        out_specs=[anywhere] * 3 + [pl.BlockSpec((8, 128), lambda c: (0, 0))],
        out_shape=[s((d // 4, ff), BF)] * 2 + [s((ff // 4, d), BF), s((8, 128), F32)],
        scratch_shapes=[pltpu.VMEM((tokens, 256), BF)] * 3 + [pltpu.VMEM((256, d), BF)] + ring_scratch(d),
        compiler_params=pltpu.CompilerParams(vmem_limit_bytes=VMEM_LIMIT, collective_id=2, has_side_effects=True),
        name="layer0",
    )(dh, dht, at0, gate, gate, up, up, wd, wd)


def adamw(w, m, v, g):
    m = 0.9 * m + 0.1 * g
    v = 0.95 * v + 0.05 * g * g
    step = m * lax.rsqrt(v + 1e-8) + 0.1 * w
    return (w - 0.02 * step).astype(BF), m, v


def solution(mesh):
    def step(x, dy, wg, wu, wd, *moments):
        x, dy = x[0], dy[0]
        gate, up, at0, h, a1, at1, dyt = forward(x, dy, wg, wu, wd)
        dgate, dup, g1, u1, d1, sq1 = layer1(a1, at1, dy, dyt, wg, wu, wd)
        dh, dht = input_gradient(dgate, dup, h, dy, wg, wu)
        g0, u0, d0, sq0 = layer0(dh, dht, at0, gate, up, wd)
        squares = lax.psum(jnp.sum(sq0) + jnp.sum(sq1), "dp")
        count = wg.size + wu.size + wd.size
        factor = jnp.minimum(1.0, 0.5 * lax.rsqrt(squares / count + 1e-30))
        me = lax.axis_index("dp")
        new = []
        for i, (w, gradient) in enumerate(((wg, (g0, g1)), (wu, (u0, u1)), (wd, (d0, d1)))):
            m, v = moments[i], moments[3 + i]
            block = lax.dynamic_slice_in_dim(w, me * m.shape[1], m.shape[1], 1)
            w, m, v = adamw(block.astype(F32), m, v, jnp.stack(gradient).astype(F32) * factor)
            new.append((lax.all_gather(w, "dp", axis=1, tiled=True), m, v))
        return tuple(one[which] for which in range(3) for one in new)

    whole, part = P(), P(None, "dp", None)
    return jax.shard_map(
        step,
        mesh=mesh,
        in_specs=(P(("rep", "dp")),) * 2 + (whole,) * 3 + (part,) * 6,
        out_specs=(P("rep"),) * 3 + (P("rep", "dp", None),) * 6,
        check_vma=False,
    )
```

```python
import functools

import jax
import jax.numpy as jnp
from jax import lax
from jax.experimental import pallas as pl
from jax.experimental.pallas import tpu as pltpu
from jax.sharding import PartitionSpec as P

BF = jnp.bfloat16
F32 = jnp.float32
VMEM_LIMIT = 67_000_000
MESH = pl.DeviceIdType.MESH
NN = (((1,), (0,)), ((), ()))
NT = (((1,), (1,)), ((), ()))
ONE = pl.Buffered(1)
STEPS = 11
TILE = 512


def dot(a, b, dims):
    return lax.dot_general(a, b, dims, preferred_element_type=F32)


def first_strip(c):
    return jnp.where(c == 10, 5, jnp.where(c % 2 == 0, c // 2, 11 + c // 2))


def second_strip(c):
    return jnp.where(c == 10, 16, jnp.where(c % 2 == 0, 6 + c // 2, 17 + c // 2))


def normed(wide):
    scale = lax.rsqrt(jnp.mean(wide * wide, -1, keepdims=True) + 1e-6)
    return (wide * scale).astype(BF), scale


def forward_kernel(x_ref, dy_ref, wg_ref, wu_ref, wd_ref, gate_ref, up_ref, at0_ref, h_ref, a1_ref, at1_ref, dyt_ref, act):
    dyt_ref[...] = dy_ref[...].T
    sub = TILE // 2
    for i in range(2):
        rows = slice(i * sub, (i + 1) * sub)
        a, _ = normed(x_ref[rows, :].astype(F32))
        at0_ref[:, rows] = a.T
        for c in range(STEPS):
            cols = slice(256 * c, 256 * (c + 1))
            gate = dot(a, wg_ref[:, cols], NN)
            up = dot(a, wu_ref[:, cols], NN)
            gate_ref[rows, cols] = gate
            up_ref[rows, cols] = up
            act[rows, cols] = (gate * jax.nn.sigmoid(gate) * up).astype(BF)
    for i in range(2):
        rows = slice(i * sub, (i + 1) * sub)
        down = dot(act[rows, :], wd_ref[...], NN).astype(BF)
        h = (x_ref[rows, :].astype(F32) + down.astype(F32)).astype(BF)
        h_ref[rows, :] = h
        a1, _ = normed(h.astype(F32))
        a1_ref[rows, :] = a1
        at1_ref[:, rows] = a1.T


def forward(x, dy, wg, wu, wd):
    tokens, d = x.shape
    ff = wg.shape[2]
    row = pl.BlockSpec((TILE, d), lambda i: (i, 0))
    col = pl.BlockSpec((d, TILE), lambda i: (0, i))
    wide = pl.BlockSpec((TILE, ff), lambda i: (i, 0))
    up_spec = pl.BlockSpec((None, d, ff), lambda i: (0, 0, 0), pipeline_mode=ONE)
    down_spec = pl.BlockSpec((None, ff, d), lambda i: (0, 0, 0), pipeline_mode=ONE)
    s = jax.ShapeDtypeStruct
    return pl.pallas_call(
        forward_kernel,
        grid=(tokens // TILE,),
        in_specs=[row, row, up_spec, up_spec, down_spec],
        out_specs=[wide, wide, col, row, row, col, col],
        out_shape=[s((tokens, ff), F32), s((tokens, ff), F32), s((d, tokens), BF), s((tokens, d), BF), s((tokens, d), BF), s((d, tokens), BF), s((d, tokens), BF)],
        scratch_shapes=[pltpu.VMEM((TILE, ff), BF)],
        compiler_params=pltpu.CompilerParams(vmem_limit_bytes=VMEM_LIMIT),
        name="fwd0",
    )(x, dy, wg, wu, wd)


class Ring:
    def __init__(self, item, rows, refs, emit):
        self.item = item
        self.rows = rows
        self.term, self.recv, self.send, self.fin, self.ssem, self.rsem, self.fsem, self.total = refs
        self.emit = emit

    def copy(self, h, d, k, half):
        me = lax.axis_index("dp")
        to = lax.rem(me + (1 if d == 0 else 3), 4)
        slot = lax.rem(k, 2)
        if h == 0:
            src = self.term.at[lax.rem(k, self.term.shape[0]), pl.ds(self.start(h, d, half, True), half), :]
        else:
            src = self.send.at[h - 1, d, slot, pl.ds(0, half), :]
        return pltpu.make_async_remote_copy(
            src_ref=src,
            dst_ref=self.recv.at[h, d, slot, pl.ds(0, half), :],
            send_sem=self.ssem.at[h, d, slot],
            recv_sem=self.rsem.at[h, d, slot],
            device_id={"dp": to},
            device_id_type=MESH,
        )

    def start(self, h, d, half, sending):
        me = lax.axis_index("dp")
        away = h + 1 if sending else h + 2
        block = lax.rem(me + 8 - away, 4) if d == 0 else lax.rem(me + away, 4)
        return pl.multiple_of(block * 2 * half + d * half, half)

    def each(self, t, body):
        there, k = self.item(t)
        for condition, half in self.rows:
            where = there if condition is None else jnp.logical_and(there, condition(k))
            pl.when(where)(functools.partial(body, k, half))

    def point(self, t):
        def arrived(h, k, half):
            for d in range(2):
                self.copy(h, d, k, half).wait()

        def add(h, k, half):
            slot = lax.rem(k, 2)
            for d in range(2):
                mine = self.term[lax.rem(k, self.term.shape[0]), pl.ds(self.start(h, d, half, False), half), :]
                value = (self.recv[h, d, slot, pl.ds(0, half), :].astype(F32) + mine.astype(F32)).astype(BF)
                if h < 2:
                    self.send[h, d, slot, pl.ds(0, half), :] = value
                else:
                    self.fin[slot, pl.ds(d * half, half), :] = value
                    wide = value.astype(F32)
                    square = wide * wide
                    parts = [square[:, 128 * i : 128 * (i + 1)] for i in range(square.shape[1] // 128)]
                    part = functools.reduce(jnp.add, parts)
                    self.total[...] += jnp.sum(part.reshape(half // 8, 8, 128), 0)

        def leave(h, k, half):
            for d in range(2):
                self.copy(h, d, k, half).start()

        def out(k, half):
            for c in self.emit(k, lax.rem(k, 2), 2 * half):
                c.start()

        def gone(k, half):
            for c in self.emit(k, lax.rem(k, 2), 2 * half):
                c.wait()

        for h in range(3):
            self.each(t - 1 - h, functools.partial(arrived, h))
        self.each(t - 4, gone)
        for h in range(3):
            self.each(t - 1 - h, functools.partial(add, h))
        for h in range(3):
            self.each(t - h, functools.partial(leave, h))
        self.each(t - 3, out)


def rings(c_refs, g_out, u_out, d_out):
    (g_term, u_term, d_term, g_recv, u_recv, d_recv, g_send, u_send, d_send, g_fin, u_fin, d_fin, ssem, rsem, fsem, total) = c_refs
    me = lax.axis_index("dp")

    def every(t):
        return jnp.logical_and(t >= 0, t < STEPS), t

    def pairs(t):
        last = t == 11
        return jnp.logical_or(last, jnp.logical_and(jnp.logical_and(t >= 2, t <= 10), lax.rem(t, 2) == 0)), jnp.where(last, 5, lax.div(t - 2, 2))

    def strips(fin, out, sem):
        def emit(k, slot, rows):
            return [
                pltpu.make_async_copy(
                    fin.at[slot, :, pl.ds(128 * i, 128)], out.at[:, pl.ds(pl.multiple_of(128 * strip(k), 128), 128)], sem.at[slot, i]
                )
                for i, strip in enumerate((first_strip, second_strip))
            ]

        return emit

    def down(k, slot, rows):
        odd = lax.rem(me, 2)
        at = 128 * k + 64 * odd if rows == 128 else 640 * (1 - odd)
        return [pltpu.make_async_copy(d_fin.at[slot, pl.ds(0, rows), :], d_out.at[pl.ds(pl.multiple_of(at, 64), rows), :], fsem.at[2, slot, 0])]

    g = Ring(every, [(None, 128)], (g_term, g_recv, g_send, g_fin, ssem.at[0], rsem.at[0], None, total), strips(g_fin, g_out, fsem.at[0]))
    u = Ring(every, [(None, 128)], (u_term, u_recv, u_send, u_fin, ssem.at[1], rsem.at[1], None, total), strips(u_fin, u_out, fsem.at[1]))
    d = Ring(
        pairs, [(lambda k: k < 5, 64), (lambda k: k == 5, 32)], (d_term, d_recv, d_send, d_fin, ssem.at[2], rsem.at[2], None, total), down
    )
    return g, u, d


def ring_scratch(d):
    v = pltpu.VMEM
    return [
        v((4, d, 256), BF),
        v((4, d, 256), BF),
        v((3, 512, d), BF),
        v((3, 2, 2, 128, 256), BF),
        v((3, 2, 2, 128, 256), BF),
        v((3, 2, 2, 64, d), BF),
        v((2, 2, 2, 128, 256), BF),
        v((2, 2, 2, 128, 256), BF),
        v((2, 2, 2, 64, d), BF),
        v((2, 256, 256), BF),
        v((2, 256, 256), BF),
        v((2, 128, d), BF),
        pltpu.SemaphoreType.DMA((3, 3, 2, 2)),
        pltpu.SemaphoreType.DMA((3, 3, 2, 2)),
        pltpu.SemaphoreType.DMA((3, 2, 2)),
        v((8, 128), F32),
    ]


def greet():
    me = lax.axis_index("dp")
    barrier = pltpu.get_barrier_semaphore()
    for other in (lax.rem(me + 1, 4), lax.rem(me + 3, 4)):
        pl.semaphore_signal(barrier, inc=1, device_id={"dp": other}, device_id_type=MESH)
    pl.semaphore_wait(barrier, 2)


def split(out, left, right, n):
    rows = left.shape[0] // n
    for i in range(n):
        out[rows * i : rows * (i + 1), :] = dot(left[rows * i : rows * (i + 1), :], right[...], NN).astype(BF)


def weight_gradients(c, at_ref, dyt_ref, dg, du, act, c_refs, g, u, d):
    g_term, u_term, d_term = c_refs[:3]
    split(g_term.at[lax.rem(c, 4)], at_ref, dg, 2)
    split(u_term.at[lax.rem(c, 4)], at_ref, du, 2)
    g.point(c)
    down = jnp.concatenate([dot(dyt_ref[1024 // 2 * i : 1024 // 2 * (i + 1), :], act[...], NN).astype(BF).T for i in range(2)], 1)
    half = c // 2
    d_term[lax.rem(half, 3), pl.ds(pl.multiple_of(256 * lax.rem(c, 2), 256), 256), :] = down
    u.point(c)


def drain(c, c_refs, g, u, d, sq_ref):
    @pl.when(c == STEPS - 1)
    def _():
        def one(t, _):
            d.point(t)
            g.point(t)
            u.point(t)
            return 0

        lax.fori_loop(STEPS, STEPS + 5, one, 0)
        sq_ref[...] = c_refs[-1][...]


def layer1_kernel(a_ref, at_ref, dy_ref, dyt_ref, wg1, wg2, wu1, wu2, wd1, wd2, dgate_out, dup_out, g_out, u_out, d_out, sq_ref, act, dg, du, wg, wu, wd, osem, *c_refs):
    c = pl.program_id(0)
    g, u, d = rings(c_refs, g_out, u_out, d_out)

    def put(k):
        cols = pl.ds(pl.multiple_of(256 * k, 256), 256)
        return [pltpu.make_async_copy(dg, dgate_out.at[:, cols], osem.at[0]), pltpu.make_async_copy(du, dup_out.at[:, cols], osem.at[1])]

    @pl.when(c == 0)
    def _():
        greet()
        c_refs[-1][...] = jnp.zeros((8, 128), F32)

    wg[:, :128] = wg1[...]
    wg[:, 128:] = wg2[...]
    wu[:, :128] = wu1[...]
    wu[:, 128:] = wu2[...]
    wd[:128, :] = wd1[...]
    wd[128:, :] = wd2[...]

    @pl.when(c > 0)
    def _():
        for p in put(c - 1):
            p.wait()

    for i in range(a_ref.shape[0] // TILE):
        rows = slice(i * TILE, (i + 1) * TILE)
        gate = dot(a_ref[rows, :], wg[...], NN)
        up = dot(a_ref[rows, :], wu[...], NN)
        dact = dot(dy_ref[rows, :], wd[...], NT).astype(BF).astype(F32)
        s = jax.nn.sigmoid(gate)
        silu = gate * s
        act[rows, :] = (silu * up).astype(BF)
        du[rows, :] = (dact * silu).astype(BF)
        dg[rows, :] = (dact * up * (s + silu * (1.0 - s))).astype(BF)
    d.point(c)
    for p in put(c):
        p.start()
    weight_gradients(c, at_ref, dyt_ref, dg, du, act, c_refs, g, u, d)
    drain(c, c_refs, g, u, d, sq_ref)

    @pl.when(c == STEPS - 1)
    def _():
        for p in put(c):
            p.wait()


def layer1(a1, at1, dy, dyt, wg, wu, wd):
    tokens, d = a1.shape
    ff = wg.shape[2]
    s = jax.ShapeDtypeStruct
    whole = lambda shape: pl.BlockSpec(shape, lambda c: (0, 0), pipeline_mode=ONE)
    cols = lambda strip: pl.BlockSpec((None, d, 128), lambda c: (1, 0, strip(c)))
    rows = lambda strip: pl.BlockSpec((None, 128, d), lambda c: (1, strip(c), 0))
    anywhere = pl.BlockSpec(memory_space=pl.ANY)
    return pl.pallas_call(
        layer1_kernel,
        grid=(STEPS,),
        in_specs=[whole((tokens, d)), whole((d, tokens)), whole((tokens, d)), whole((d, tokens))]
        + [cols(first_strip), cols(second_strip)] * 2
        + [rows(first_strip), rows(second_strip)],
        out_specs=[anywhere] * 5 + [pl.BlockSpec((8, 128), lambda c: (0, 0))],
        out_shape=[s((tokens, ff), BF)] * 2 + [s((d // 4, ff), BF)] * 2 + [s((ff // 4, d), BF), s((8, 128), F32)],
        scratch_shapes=[pltpu.VMEM((tokens, 256), BF)] * 3
        + [pltpu.VMEM((d, 256), BF)] * 2
        + [pltpu.VMEM((256, d), BF), pltpu.SemaphoreType.DMA((2,))]
        + ring_scratch(d),
        compiler_params=pltpu.CompilerParams(vmem_limit_bytes=VMEM_LIMIT, collective_id=1, has_side_effects=True),
        name="layer1",
    )(a1, at1, dy, dyt, wg, wg, wu, wu, wd, wd)


def input_kernel(dg_ref, du_ref, h_ref, dy_ref, wg_any, wu_any, dh_ref, dht_ref, wg, wu, sem):
    def fetch():
        copies = []
        for which, (src, dst) in enumerate(((wg_any, wg), (wu_any, wu))):
            for c in range(STEPS):
                strips = (5, 16) if c == 10 else ((c // 2, 6 + c // 2) if c % 2 == 0 else (11 + c // 2, 17 + c // 2))
                for i, strip in enumerate(strips):
                    copies.append(
                        pltpu.make_async_copy(
                            src.at[1, :, pl.ds(128 * strip, 128)], dst.at[:, pl.ds(256 * c + 128 * i, 128)], sem.at[which, 2 * c + i]
                        )
                    )
        return copies

    @pl.when(pl.program_id(0) == 0)
    def _():
        copies = fetch()
        for c in copies:
            c.start()
        for c in copies:
            c.wait()

    sub = TILE // 2
    for i in range(2):
        rows = slice(i * sub, (i + 1) * sub)
        da = dot(dg_ref[rows, :], wg[...], NT).astype(BF).astype(F32) + dot(du_ref[rows, :], wu[...], NT).astype(BF).astype(F32)
        da = da.astype(BF).astype(F32)
        wide = h_ref[rows, :].astype(F32)
        scale = lax.rsqrt(jnp.mean(wide * wide, -1, keepdims=True) + 1e-6)
        along = jnp.sum(da * wide, -1, keepdims=True) * (scale * scale * scale) * (1.0 / wide.shape[-1])
        back = (da * scale - wide * along).astype(BF)
        dh = (dy_ref[rows, :].astype(F32) + back.astype(F32)).astype(BF)
        dh_ref[rows, :] = dh
        dht_ref[:, rows] = dh.T


def input_gradient(dg, du, h, dy, wg, wu):
    tokens, d = h.shape
    ff = dg.shape[1]
    row = pl.BlockSpec((TILE, d), lambda i: (i, 0))
    wide = pl.BlockSpec((TILE, ff), lambda i: (i, 0))
    anywhere = pl.BlockSpec(memory_space=pl.ANY)
    s = jax.ShapeDtypeStruct
    return pl.pallas_call(
        input_kernel,
        grid=(tokens // TILE,),
        in_specs=[wide, wide, row, row, anywhere, anywhere],
        out_specs=[row, pl.BlockSpec((d, TILE), lambda i: (0, i))],
        out_shape=[s((tokens, d), BF), s((d, tokens), BF)],
        scratch_shapes=[pltpu.VMEM((d, ff), BF)] * 2 + [pltpu.SemaphoreType.DMA((2, 22))],
        compiler_params=pltpu.CompilerParams(vmem_limit_bytes=VMEM_LIMIT),
        name="input1",
    )(dg, du, h, dy, wg, wu)


def layer0_kernel(dh_ref, dht_ref, at_ref, g1, g2, u1, u2, wd1, wd2, g_out, u_out, d_out, sq_ref, act, dg, du, wd, *c_refs):
    c = pl.program_id(0)
    g, u, d = rings(c_refs, g_out, u_out, d_out)

    @pl.when(c == 0)
    def _():
        greet()
        c_refs[-1][...] = jnp.zeros((8, 128), F32)

    wd[:128, :] = wd1[...]
    wd[128:, :] = wd2[...]
    for i in range(dh_ref.shape[0] // TILE):
        rows = slice(i * TILE, (i + 1) * TILE)
        dact_all = dot(dh_ref[rows, :], wd[...], NT).astype(BF).astype(F32)
        for j, (gate_ref, up_ref) in enumerate(((g1, u1), (g2, u2))):
            cols = slice(128 * j, 128 * (j + 1))
            dact, gate, up = dact_all[:, cols], gate_ref[rows, :], up_ref[rows, :]
            s = jax.nn.sigmoid(gate)
            silu = gate * s
            act[rows, cols] = (silu * up).astype(BF)
            du[rows, cols] = (dact * silu).astype(BF)
            dg[rows, cols] = (dact * up * (s + silu * (1.0 - s))).astype(BF)
    d.point(c)
    weight_gradients(c, at_ref, dht_ref, dg, du, act, c_refs, g, u, d)
    drain(c, c_refs, g, u, d, sq_ref)


def layer0(dh, dht, at0, gate, up, wd):
    tokens, d = dh.shape
    ff = gate.shape[1]
    s = jax.ShapeDtypeStruct
    whole = lambda shape: pl.BlockSpec(shape, lambda c: (0, 0), pipeline_mode=ONE)
    wide = lambda strip: pl.BlockSpec((tokens, 128), lambda c: (0, strip(c)))
    rows = lambda strip: pl.BlockSpec((None, 128, d), lambda c: (0, strip(c), 0))
    anywhere = pl.BlockSpec(memory_space=pl.ANY)
    return pl.pallas_call(
        layer0_kernel,
        grid=(STEPS,),
        in_specs=[whole((tokens, d)), whole((d, tokens)), whole((d, tokens))]
        + [wide(first_strip), wide(second_strip)] * 2
        + [rows(first_strip), rows(second_strip)],
        out_specs=[anywhere] * 3 + [pl.BlockSpec((8, 128), lambda c: (0, 0))],
        out_shape=[s((d // 4, ff), BF)] * 2 + [s((ff // 4, d), BF), s((8, 128), F32)],
        scratch_shapes=[pltpu.VMEM((tokens, 256), BF)] * 3 + [pltpu.VMEM((256, d), BF)] + ring_scratch(d),
        compiler_params=pltpu.CompilerParams(vmem_limit_bytes=VMEM_LIMIT, collective_id=2, has_side_effects=True),
        name="layer0",
    )(dh, dht, at0, gate, gate, up, up, wd, wd)


def moments_of(m, v, g):
    return 0.9 * m + 0.1 * g, 0.95 * v + 0.05 * g * g


def weight_of(w, m, v):
    return (w - 0.02 * (m * lax.rsqrt(v + 1e-8) + 0.1 * w)).astype(BF)


def gather_kernel(count, sq0, sq1, mg, vg, mu, vu, md, vd, wg, wu, wd, g0, g1, u0, u1, d0, d1, wg_all, wu_all, wd_all, own, factor_ref, *scratch):
    (stage_g, stage_u, stage_d, stage_own, m_up, v_up, w_up, g_up, m_dn, v_dn, w_dn, g_dn, sums, total, load, local, near_s, near_r, far_s, far_r, sum_s, sum_r, sum_l) = scratch
    me = lax.axis_index("dp")
    right, left, across = lax.rem(me + 1, 4), lax.rem(me + 3, 4), lax.rem(me + 2, 4)

    up_buf, down_buf = (m_up, v_up, w_up, g_up), (m_dn, v_dn, w_dn, g_dn)
    gate = (mg, vg, wg, (g0, g1), wg_all, stage_g, up_buf, 0, 4, 0, 8, 64)
    up = (mu, vu, wu, (u0, u1), wu_all, stage_u, up_buf, 8, 4, 0, 8, 64)
    down0 = (md, vd, wd, (d0, d1), wd_all, stage_d, down_buf, 16, 2, 0, 2, 352)
    down1 = (md, vd, wd, (d0, d1), own, stage_own, down_buf, 18, 2, 2, 2, 352)

    def where(matrix, i):
        _, _, _, _, _, _, _, _, per, skip, _, rows = matrix
        layer = lax.div(i + skip, per)
        return layer, lax.rem(i, per) * rows

    def place(matrix, i, block, at, rows):
        layer, row = where(matrix, i)
        if matrix is down1:
            return own.at[pl.ds(pl.multiple_of(row, 16), rows), :]
        start = pl.multiple_of(block * (matrix[8] * matrix[11]) + row + at, 16)
        if matrix is down0:
            return wd_all.at[pl.ds(start, rows), :]
        return matrix[4].at[layer, pl.ds(start, rows), :]

    def loads(matrix, i, gradient):
        m, v, w, _, _, _, bufs, _, per, _, _, rows = matrix
        layer, row = where(matrix, i)
        slot = lax.rem(i, 2)
        mine = pl.ds(pl.multiple_of(row, 16), rows)
        theirs = pl.ds(pl.multiple_of(me * (per * rows) + row, 16), rows)
        sources = (m.at[layer, mine, :], v.at[layer, mine, :], w.at[layer, theirs, :], gradient.at[mine, :])
        return [pltpu.make_async_copy(s, b.at[slot], load.at[j, slot]) for j, (s, b) in enumerate(zip(sources, bufs))]

    def fetch(matrix, i):
        layer, _ = where(matrix, i)
        for n in range(2):

            @pl.when(layer == n)
            def _():
                for c in loads(matrix, i, matrix[3][n]):
                    c.start()

    def near(matrix, i, d):
        p = matrix[7] + i
        return pltpu.make_async_remote_copy(
            src_ref=matrix[5].at[i],
            dst_ref=place(matrix, i, me, 0, matrix[11]),
            send_sem=near_s.at[p, d],
            recv_sem=near_r.at[p, d],
            device_id={"dp": right if d == 0 else left},
            device_id_type=MESH,
        )

    def far(matrix, i, d):
        p = matrix[7] + i
        half = matrix[11] // 2
        spot = place(matrix, i, left if d == 0 else right, d * half, half)
        return pltpu.make_async_remote_copy(
            src_ref=spot,
            dst_ref=spot,
            send_sem=far_s.at[p, d],
            recv_sem=far_r.at[p, d],
            device_id={"dp": right if d == 0 else left},
            device_id_type=MESH,
        )

    def keep(matrix, i):
        return pltpu.make_async_copy(matrix[5].at[i], place(matrix, i, me, 0, matrix[11]), local.at[matrix[7] + i])

    fetch(gate, 0)
    barrier = pltpu.get_barrier_semaphore()
    for other in (right, left, across):
        pl.semaphore_signal(barrier, inc=1, device_id={"dp": other}, device_id_type=MESH)
    pl.semaphore_wait(barrier, 3)

    def share(which, j):
        return pltpu.make_async_remote_copy(
            src_ref=(sq0, sq1)[which],
            dst_ref=sums.at[which, j + 1],
            send_sem=sum_s.at[which, j],
            recv_sem=sum_r.at[which, j],
            device_id={"dp": lax.rem(me + j + 1, 4)},
            device_id_type=MESH,
        )

    mine = [pltpu.make_async_copy(s, sums.at[n, 0], sum_l.at[n]) for n, s in enumerate((sq0, sq1))]
    for n in range(2):
        mine[n].start()
        for j in range(3):
            share(n, j).start()
    for n in range(2):
        mine[n].wait()
        for j in range(3):
            share(n, j).wait()
    parts = [sums[0, lax.rem(me + 4 - b, 4)] + sums[1, lax.rem(me + 4 - b, 4)] for b in range(4)]
    squares = jnp.sum(parts[0] + parts[1] + parts[2] + parts[3], keepdims=True)
    factor = jnp.minimum(1.0, 0.5 * lax.rsqrt(squares / count + 1e-30))
    total[...] = jnp.broadcast_to(factor, total.shape)
    factor_ref[...] = jnp.broadcast_to(factor, total.shape)

    def run(matrix, first, send):
        m_buf, v_buf, w_buf, g_buf = matrix[6]
        pieces, rows = matrix[10], matrix[11]
        if not first:
            fetch(matrix, 0)

        def body(i, _):
            slot = lax.rem(i, 2)

            @pl.when(i + 1 < pieces)
            def _():
                fetch(matrix, i + 1)

            for c in loads(matrix, i, matrix[3][0]):
                c.wait()
            f = total[0:1, 0:1]

            def some(r, _):
                at = pl.ds(pl.multiple_of(r * 16, 16), 16)
                m, v = moments_of(m_buf[slot, at, :], v_buf[slot, at, :], g_buf[slot, at, :].astype(F32) * f)
                matrix[5][i, at, :] = weight_of(w_buf[slot, at, :].astype(F32), m, v)
                return 0

            lax.fori_loop(0, rows // 16, some, 0)
            keep(matrix, i).start()
            if send:
                for d in range(2):
                    near(matrix, i, d).start()
            return 0

        lax.fori_loop(0, pieces, body, 0)

    run(gate, True, True)
    run(up, False, True)
    run(down0, False, True)
    run(down1, False, False)

    for matrix in (gate, up, down0):

        def onward(i, _):
            for d in range(2):
                near(matrix, i, d).wait()
                far(matrix, i, d).start()
            return 0

        lax.fori_loop(0, matrix[10], onward, 0)
    for matrix in (gate, up, down0, down1):

        def finish(i, _):
            keep(matrix, i).wait()
            if matrix is not down1:
                for d in range(2):
                    far(matrix, i, d).wait()
            return 0

        lax.fori_loop(0, matrix[10], finish, 0)


def gather(sq, moments, weights, gradients):
    mg, mu, md, vg, vu, vd = moments
    wg, wu, wd = weights
    _, d, ff = wg.shape
    part_up, part_dn = d // 4, ff // 4
    anywhere = pl.BlockSpec(memory_space=pl.ANY)
    s = jax.ShapeDtypeStruct
    v = pltpu.VMEM
    dma = pltpu.SemaphoreType.DMA
    return pl.pallas_call(
        functools.partial(gather_kernel, float(wg.size + wu.size + wd.size)),
        in_specs=[anywhere] * 17,
        out_specs=[anywhere] * 4 + [pl.BlockSpec(memory_space=pltpu.VMEM)],
        out_shape=[s(wg.shape, BF), s(wu.shape, BF), s((ff, d), BF), s((part_dn, d), BF), s((8, 128), F32)],
        scratch_shapes=[v((8, 64, ff), BF)] * 2
        + [v((2, part_dn // 2, d), BF)] * 2
        + [v((2, 64, ff), F32)] * 2
        + [v((2, 64, ff), BF)] * 2
        + [v((2, part_dn // 2, d), F32)] * 2
        + [v((2, part_dn // 2, d), BF)] * 2
        + [v((2, 4, 8, 128), F32), v((8, 128), F32), dma((4, 2)), dma((20,))]
        + [dma((18, 2))] * 4
        + [dma((2, 3)), dma((2, 3)), dma((2,))],
        compiler_params=pltpu.CompilerParams(vmem_limit_bytes=VMEM_LIMIT, collective_id=3, has_side_effects=True),
        name="gather",
    )(*sq, mg, vg, mu, vu, md, vd, wg, wu, wd, *gradients)


def settle_kernel(factor_ref, *refs):
    ins, outs = refs[: len(refs) * 5 // 8], refs[len(refs) * 5 // 8 :]
    first = pl.program_id(0) < 4
    f = factor_ref[0:1, 0:1]
    for n in range(len(ins) // 5):
        m, v, g0, g1, w = ins[5 * n : 5 * n + 5]
        m_out, v_out, w_out = outs[3 * n : 3 * n + 3]
        rows = m.shape[1]

        def some(r, _):
            at = pl.ds(pl.multiple_of(r * 16, 16), 16)
            g = jnp.where(first, g0[at, :].astype(F32), g1[at, :].astype(F32))
            m_out[0, at, :], v_out[0, at, :] = moments_of(m[0, at, :], v[0, at, :], g * f)
            return 0

        lax.fori_loop(0, rows // 16, some, 0)
        if len(w.shape) == 3:
            w_out[...] = w[...]
        else:

            @pl.when(first)
            def _():
                w_out[0] = w[...]


def settle(factor, matrices):
    s = jax.ShapeDtypeStruct
    in_specs, out_specs, out_shape, args = [pl.BlockSpec((8, 128), lambda i: (0, 0))], [], [], [factor]
    for m, v, a, b, w in matrices:
        _, rows, cols = m.shape
        part = pl.BlockSpec((1, rows // 4, cols), lambda i: (i // 4, i % 4, 0))
        one = pl.BlockSpec((rows // 4, cols), lambda i: (jnp.minimum(i, 3), 0))
        two = pl.BlockSpec((rows // 4, cols), lambda i: (jnp.maximum(i - 4, 0), 0))
        whole = pl.BlockSpec((1, rows, cols), lambda i: (i // 4, i % 4, 0))
        if w.ndim == 3:
            in_specs += [part, part, one, two, whole]
            out_specs += [part, part, whole]
            out_shape += [s(m.shape, F32), s(v.shape, F32), s(w.shape, BF)]
        else:
            in_specs += [part, part, one, two, pl.BlockSpec((rows, cols), lambda i: (jnp.minimum(i, 3), 0))]
            out_specs += [part, part, pl.BlockSpec((1, rows, cols), lambda i: (0, jnp.minimum(i, 3), 0))]
            out_shape += [s(m.shape, F32), s(v.shape, F32), s((2, *w.shape), BF)]
        args += [m, v, a, b, w]
    moved = sum(a.size * a.dtype.itemsize for a in args) + sum(a.size * a.dtype.itemsize for a in out_shape)
    return pl.pallas_call(
        settle_kernel,
        grid=(8,),
        in_specs=in_specs,
        out_specs=out_specs,
        out_shape=out_shape,
        compiler_params=pltpu.CompilerParams(vmem_limit_bytes=VMEM_LIMIT),
        cost_estimate=pl.CostEstimate(flops=moved * 300, bytes_accessed=moved, transcendentals=0),
        name="settle",
    )(*args)


def place_kernel(own, from_left, from_right, first, second, _, out, sem):
    me = lax.axis_index("dp")
    rows = own.shape[0]
    half = rows // 2
    copies = []
    for src, block, at, n in ((own, me, 0, rows), (from_left, me + 3, 0, rows), (from_right, me + 1, 0, rows), (first, me + 2, 0, half), (second, me + 2, half, half)):
        start = pl.multiple_of(lax.rem(block, 4) * rows + at, 16)
        copies.append(pltpu.make_async_copy(src, out.at[1, pl.ds(start, n), :], sem.at[len(copies)]))
    for c in copies:
        c.start()
    for c in copies:
        c.wait()


def place(blocks, out):
    anywhere = pl.BlockSpec(memory_space=pl.ANY)
    vmem = pl.BlockSpec(memory_space=pltpu.VMEM)
    return pl.pallas_call(
        place_kernel,
        in_specs=[vmem] * 5 + [anywhere],
        out_specs=anywhere,
        out_shape=jax.ShapeDtypeStruct(out.shape, out.dtype),
        scratch_shapes=[pltpu.SemaphoreType.DMA((5,))],
        input_output_aliases={5: 0},
        compiler_params=pltpu.CompilerParams(vmem_limit_bytes=VMEM_LIMIT),
        name="place",
    )(*blocks, out)


def solution(mesh):
    def step(x, dy, wg, wu, wd, *moments):
        x, dy = x[0], dy[0]
        gate, up, at0, h, a1, at1, dyt = forward(x, dy, wg, wu, wd)
        dgate, dup, g1, u1, d1, sq1 = layer1(a1, at1, dy, dyt, wg, wu, wd)
        dh, dht = input_gradient(dgate, dup, h, dy, wg, wu)
        g0, u0, d0, sq0 = layer0(dh, dht, at0, gate, up, wd)
        gradients = (g0, g1, u0, u1, d0, d1)
        *gathered, own, factor = gather((sq0, sq1), moments, (wg, wu, wd), gradients)
        to_right, to_left = [(i, (i + 1) % 4) for i in range(4)], [(i, (i + 3) % 4) for i in range(4)]
        half = own.shape[0] // 2
        from_left, from_right = lax.ppermute(own, "dp", to_right), lax.ppermute(own, "dp", to_left)
        (mg, mu, md, vg, vu, vd), (all_g, all_u, all_d) = moments, gathered
        mg, vg, new_g, mu, vu, new_u = settle(factor, ((mg, vg, g0, g1, all_g), (mu, vu, u0, u1, all_u)))
        from_left, from_right, new_g, factor = lax.optimization_barrier((from_left, from_right, new_g, factor))
        first, second = lax.ppermute(from_left[:half], "dp", to_right), lax.ppermute(from_right[half:], "dp", to_left)
        md, vd, new_d = settle(factor, ((md, vd, d0, d1, all_d),))
        new_d = place((own, from_left, from_right, first, second), new_d)
        return new_g, new_u, new_d, mg, mu, md, vg, vu, vd

    whole, part = P(), P(None, "dp", None)
    return jax.shard_map(
        step,
        mesh=mesh,
        in_specs=(P(("rep", "dp")),) * 2 + (whole,) * 3 + (part,) * 6,
        out_specs=(P("rep"),) * 3 + (P("rep", "dp", None),) * 6,
        check_vma=False,
    )
```

```python
import functools

import jax
import jax.numpy as jnp
from jax import lax
from jax.experimental import pallas as pl
from jax.experimental.pallas import tpu as pltpu
from jax.sharding import PartitionSpec as P

BF = jnp.bfloat16
F32 = jnp.float32
VMEM = pltpu.VMEM
DMA = pltpu.SemaphoreType.DMA
NN = (((1,), (0,)), ((), ()))
NT = (((1,), (1,)), ((), ()))
ONE = pl.Buffered(1)
ANY = pl.BlockSpec(memory_space=pl.ANY)
ALL = ...
LANES = 128
CHUNK = 256
STEPS = 11
LAST = STEPS - 1
TILE = 512
GROUP = 4
HOPS = GROUP - 1
EARLY = 576
LATE = 128


def shape(dims, dtype=BF):
    return jax.ShapeDtypeStruct(dims, dtype)


def params(collective_id=None):
    limit = 67_000_000
    if collective_id is None:
        return pltpu.CompilerParams(vmem_limit_bytes=limit)
    return pltpu.CompilerParams(vmem_limit_bytes=limit, collective_id=collective_id, has_side_effects=True)


def dot(a, b, dims):
    return lax.dot_general(a, b, dims, preferred_element_type=F32)


def span(start, size, multiple=16):
    return pl.ds(pl.multiple_of(start, multiple), size)


def local(src, dst, sem):
    return pltpu.make_async_copy(src, dst, sem)


def remote(src, dst, sent, received, to, axis="dp"):
    return pltpu.make_async_remote_copy(
        src_ref=src, dst_ref=dst, send_sem=sent, recv_sem=received, device_id={axis: to}, device_id_type=pl.DeviceIdType.MESH
    )


def around():
    me = lax.axis_index("dp")
    return (me, *(lax.rem(me + away, GROUP) for away in (1, HOPS, 2)))


def partner():
    rep = lax.axis_index("rep")
    return rep + 1 - 2 * lax.rem(rep, 2)


def greet(devices, groups=()):
    barrier = pltpu.get_barrier_semaphore()
    for axis, others in (("dp", devices), ("rep", groups)):
        for other in others:
            pl.semaphore_signal(barrier, inc=1, device_id={axis: other}, device_id_type=pl.DeviceIdType.MESH)
    pl.semaphore_wait(barrier, len(devices) + len(groups))


def start(copies):
    for c in copies:
        c.start()


def wait(copies):
    for c in copies:
        c.wait()


def first_strip(c):
    return jnp.where(c == LAST, 5, jnp.where(c % 2 == 0, c // 2, STEPS + c // 2))


def second_strip(c):
    return jnp.where(c == LAST, 16, jnp.where(c % 2 == 0, c // 2 + 6, c // 2 + 17))


def normed(wide):
    scale = lax.rsqrt(jnp.mean(wide * wide, -1, keepdims=True) + 1e-6)
    return (wide * scale).astype(BF), scale


def spread(source, dest, near_s, near_r, far_s, far_r, rows):
    me, right, left, _ = around()
    half = rows // 2
    to = (right, left)

    def near(d, n):
        part = n if d == 0 else 1 - n
        return remote(source.at[span(part * half, half), :], dest.at[span(me * rows + part * half, half), :], near_s.at[d, n], near_r.at[d, n], to[d])

    def far(d):
        spot = dest.at[span((left, right)[d] * rows + d * half, half), :]
        return remote(spot, spot, far_s.at[d], far_r.at[d], to[d])

    ways = range(2)
    return [near(d, 0) for d in ways], [near(d, 1) for d in ways], [far(d) for d in ways]


def spread_scratch():
    return [DMA((2, 2)), DMA((2, 2)), DMA((2,)), DMA((2,)), DMA((2,))]


def forward_kernel(x_ref, dy_ref, wg_ref, wu_ref, wd_ref, m_ref, v_ref, gate_ref, up_ref, at0_ref, h_ref, a1_ref, at1_ref, dyt_ref, mine_ref, act, moment, *sems):
    step = pl.program_id(0)
    me, right, left, _ = around()
    kind = lax.rem(lax.axis_index("rep"), 2)
    bounce = sems[-1]
    to_stage = [local(ref.at[1, pl.ds(0, EARLY), :], moment, bounce.at[0]) for ref in (m_ref, v_ref)]
    from_stage = local(moment, mine_ref.at[span(me * EARLY, EARLY), :], bounce.at[1])
    near0, near1, far = spread(moment, mine_ref, *sems[:-1], EARLY)

    @pl.when(step == 0)
    def _():
        for n, copy in enumerate(to_stage):
            pl.when(kind == n)(copy.start)
        greet((right, left))
        to_stage[0].wait()
        start(near0 + near1 + [from_stage])

    @pl.when(step == 5)
    def _():
        from_stage.wait()
        wait(near0)
        start(far)

    dyt_ref[ALL] = dy_ref[ALL].T
    sub = TILE // 2
    for i in range(2):
        rows = slice(i * sub, (i + 1) * sub)
        a, _ = normed(x_ref[rows, :].astype(F32))
        at0_ref[:, rows] = a.T
        for c in range(STEPS):
            cols = slice(CHUNK * c, CHUNK * (c + 1))
            gate = dot(a, wg_ref[:, cols], NN)
            up = dot(a, wu_ref[:, cols], NN)
            gate_ref[rows, cols] = gate
            up_ref[rows, cols] = up
            act[rows, cols] = (gate * jax.nn.sigmoid(gate) * up).astype(BF)
    for i in range(2):
        rows = slice(i * sub, (i + 1) * sub)
        down = dot(act[rows, :], wd_ref[ALL], NN).astype(BF)
        h = (x_ref[rows, :].astype(F32) + down.astype(F32)).astype(BF)
        h_ref[rows, :] = h
        a1, _ = normed(h.astype(F32))
        a1_ref[rows, :] = a1
        at1_ref[:, rows] = a1.T

    @pl.when(step == pl.num_programs(0) - 1)
    def _():
        wait(near1 + far)


def forward(x, dy, wg, wu, wd, m, v):
    tokens, d = x.shape
    ff = wg.shape[2]
    row = pl.BlockSpec((TILE, d), lambda i: (i, 0))
    col = pl.BlockSpec((d, TILE), lambda i: (0, i))
    wide = pl.BlockSpec((TILE, ff), lambda i: (i, 0))
    up_spec = pl.BlockSpec((None, d, ff), lambda i: (0, 0, 0), pipeline_mode=ONE)
    down_spec = pl.BlockSpec((None, ff, d), lambda i: (0, 0, 0), pipeline_mode=ONE)
    across, along = shape((d, tokens)), shape((tokens, d))
    return pl.pallas_call(
        forward_kernel,
        grid=(tokens // TILE,),
        in_specs=[row, row, up_spec, up_spec, down_spec, ANY, ANY],
        out_specs=[wide, wide, col, row, row, col, col, ANY],
        out_shape=[shape((tokens, ff), F32)] * 2 + [across, along, along, across, across, shape((GROUP * EARLY, d), F32)],
        scratch_shapes=[VMEM((TILE, ff), BF), VMEM((EARLY, d), F32)] + spread_scratch(),
        compiler_params=params(4),
        name="fwd0",
    )(x, dy, wg, wu, wd, m, v)


class Ring:
    def __init__(self, item, rows, refs, emit):
        self.item = item
        self.rows = rows
        self.term, self.recv, self.send, self.fin, self.ssem, self.rsem, self.total = refs
        self.emit = emit

    def mine(self, h, d, k, half, away):
        me = lax.axis_index("dp")
        away = away + h
        block = lax.rem(me + 2 * GROUP - away, GROUP) if d == 0 else lax.rem(me + away, GROUP)
        return lax.rem(k, self.term.shape[0]), span(block * 2 * half + d * half, half, half), slice(None)

    def copy(self, h, d, k, half):
        _, right, left, _ = around()
        spot = (d, lax.rem(k, 2), pl.ds(0, half), slice(None))
        src = self.term.at[self.mine(h, d, k, half, 1)] if h == 0 else self.send.at[h - 1, *spot]
        sems = self.ssem.at[h, *spot[:2]], self.rsem.at[h, *spot[:2]]
        return remote(src, self.recv.at[h, *spot], *sems, (right, left)[d])

    def each(self, t, body):
        there, k = self.item(t)
        for condition, half in self.rows:
            where = there if condition is None else jnp.logical_and(there, condition(k))
            pl.when(where)(functools.partial(body, k, half))

    def point(self, t):
        ways = range(2)

        def arrived(h, k, half):
            wait([self.copy(h, d, k, half) for d in ways])

        def add(h, k, half):
            slot = lax.rem(k, 2)
            for d in ways:
                spot = (d, slot, pl.ds(0, half), slice(None))
                value = (self.recv[h, *spot].astype(F32) + self.term[self.mine(h, d, k, half, 2)].astype(F32)).astype(BF)
                if h < HOPS - 1:
                    self.send[h, *spot] = value
                else:
                    self.fin[slot, pl.ds(d * half, half), :] = value
                    square = value.astype(F32) ** 2
                    parts = [square[:, LANES * i : LANES * (i + 1)] for i in range(square.shape[1] // LANES)]
                    self.total[ALL] += jnp.sum(functools.reduce(jnp.add, parts).reshape(half // 8, 8, LANES), 0)

        def leave(h, k, half):
            start([self.copy(h, d, k, half) for d in ways])

        def out(k, half):
            start(self.emit(k, lax.rem(k, 2), 2 * half))

        def gone(k, half):
            wait(self.emit(k, lax.rem(k, 2), 2 * half))

        for h in range(HOPS):
            self.each(t - 1 - h, functools.partial(arrived, h))
        self.each(t - HOPS - 1, gone)
        for h in range(HOPS):
            self.each(t - 1 - h, functools.partial(add, h))
        for h in range(HOPS):
            self.each(t - h, functools.partial(leave, h))
        self.each(t - HOPS, out)


def rings(refs, g_out, u_out, d_out):
    (g_term, u_term, d_term, g_recv, u_recv, d_recv, g_send, u_send, d_send, g_fin, u_fin, d_fin, ssem, rsem, fsem, total) = refs
    me = lax.axis_index("dp")

    def every(t):
        return jnp.logical_and(t >= 0, t < STEPS), t

    def pairs(t):
        last = t == STEPS
        return jnp.logical_or(last, jnp.logical_and(jnp.logical_and(t >= 2, t < STEPS), lax.rem(t, 2) == 0)), jnp.where(last, 5, lax.div(t, 2) - 1)

    def strips(fin, out, sem):
        def emit(k, slot, rows):
            return [
                local(fin.at[slot, :, pl.ds(LANES * i, LANES)], out.at[:, span(LANES * strip(k), LANES, LANES)], sem.at[slot, i])
                for i, strip in enumerate((first_strip, second_strip))
            ]

        return emit

    def down(k, slot, rows):
        odd = lax.rem(me, 2)
        at = LANES * k + 64 * odd if rows == LANES else 640 * (1 - odd)
        return [local(d_fin.at[slot, pl.ds(0, rows), :], d_out.at[span(at, rows, 64), :], fsem.at[2, slot, 0])]

    halves = [(None, LANES)]
    return (
        Ring(every, halves, (g_term, g_recv, g_send, g_fin, ssem.at[0], rsem.at[0], total), strips(g_fin, g_out, fsem.at[0])),
        Ring(every, halves, (u_term, u_recv, u_send, u_fin, ssem.at[1], rsem.at[1], total), strips(u_fin, u_out, fsem.at[1])),
        Ring(pairs, [(lambda k: k < 5, 64), (lambda k: k == 5, 32)], (d_term, d_recv, d_send, d_fin, ssem.at[2], rsem.at[2], total), down),
    )


def ring_scratch(d):
    up, down = (2, 2, LANES, CHUNK), (2, 2, 64, d)
    return (
        [VMEM((GROUP, d, CHUNK), BF)] * 2
        + [VMEM((3, TILE, d), BF)]
        + [VMEM((HOPS, *up), BF)] * 2
        + [VMEM((HOPS, *down), BF)]
        + [VMEM((HOPS - 1, *up), BF)] * 2
        + [VMEM((HOPS - 1, *down), BF)]
        + [VMEM((2, CHUNK, CHUNK), BF)] * 2
        + [VMEM((2, LANES, d), BF), DMA((3, HOPS, 2, 2)), DMA((3, HOPS, 2, 2)), DMA((3, 2, 2)), VMEM((8, LANES), F32)]
    )


def weight_gradients(c, at_ref, dyt_ref, dg, du, act, refs, g, u, rolled):
    terms = refs[:3]
    half = at_ref.shape[0] // 2

    def cut(body):
        if rolled:
            lax.fori_loop(0, 2, lambda i, _: body(span(half * i, half)), None)
        else:
            for i in range(2):
                body(slice(half * i, half * (i + 1)))

    for term, right in zip(terms[:2], (dg, du)):

        def up(rows):
            term[lax.rem(c, GROUP), rows, :] = dot(at_ref[rows, :], right[ALL], NN).astype(BF)

        cut(up)
    g.point(c)

    def down(rows):
        value = dot(dyt_ref[rows, :], act[ALL], NN).astype(BF).T
        terms[2][lax.rem(c // 2, 3), span(CHUNK * lax.rem(c, 2), CHUNK), rows] = value

    cut(down)
    u.point(c)


def drain(c, refs, g, u, d, sq_ref):
    @pl.when(c == LAST)
    def _():
        def one(t, _):
            for ring in (d, g, u):
                ring.point(t)

        lax.fori_loop(STEPS, STEPS + HOPS + 2, one, None)
        sq_ref[ALL] = refs[-1][ALL]


def layer1_kernel(a_ref, at_ref, dy_ref, dyt_ref, wg1, wg2, wu1, wu2, wd1, wd2, mine_ref, dgate_out, dup_out, g_out, u_out, d_out, sq_ref, other_ref, act, dg, du, wg, wu, wd, osem, msem, *refs):
    c = pl.program_id(0)
    g, u, d = rings(refs, g_out, u_out, d_out)
    exchange = remote(mine_ref, other_ref, msem.at[0], msem.at[1], partner(), "rep")

    def put(k):
        cols = span(CHUNK * k, CHUNK, CHUNK)
        return [local(dg, dgate_out.at[:, cols], osem.at[0]), local(du, dup_out.at[:, cols], osem.at[1])]

    @pl.when(c == 0)
    def _():
        greet(around()[1:3], (partner(),))
        refs[-1][ALL] = jnp.zeros_like(refs[-1])

    for one, two, both in ((wg1, wg2, wg), (wu1, wu2, wu)):
        both[:, :LANES] = one[ALL]
        both[:, LANES:] = two[ALL]
    wd[:LANES, :] = wd1[ALL]
    wd[LANES:, :] = wd2[ALL]

    @pl.when(c > 0)
    def _():
        wait(put(c - 1))

    pl.when(c == 2)(exchange.start)

    for i in range(a_ref.shape[0] // TILE):
        rows = slice(i * TILE, (i + 1) * TILE)
        gate = dot(a_ref[rows, :], wg[ALL], NN)
        up = dot(a_ref[rows, :], wu[ALL], NN)
        dact = dot(dy_ref[rows, :], wd[ALL], NT).astype(BF).astype(F32)
        s = jax.nn.sigmoid(gate)
        silu = gate * s
        act[rows, :] = (silu * up).astype(BF)
        du[rows, :] = (dact * silu).astype(BF)
        dg[rows, :] = (dact * up * (s + silu * (1.0 - s))).astype(BF)
    d.point(c)
    start(put(c))
    weight_gradients(c, at_ref, dyt_ref, dg, du, act, refs, g, u, False)
    drain(c, refs, g, u, d, sq_ref)

    @pl.when(c == LAST)
    def _():
        wait([*put(c), exchange])


def strips_of(layer, d):
    cols = [pl.BlockSpec((None, d, LANES), lambda c, s=s: (layer, 0, s(c))) for s in (first_strip, second_strip)]
    rows = [pl.BlockSpec((None, LANES, d), lambda c, s=s: (layer, s(c), 0)) for s in (first_strip, second_strip)]
    return cols, rows


def layer1(a1, at1, dy, dyt, wg, wu, wd, mine):
    tokens, d = a1.shape
    ff = wg.shape[2]
    along, across = (pl.BlockSpec(s, lambda c: (0, 0), pipeline_mode=ONE) for s in ((tokens, d), (d, tokens)))
    cols, rows = strips_of(1, d)
    return pl.pallas_call(
        layer1_kernel,
        grid=(STEPS,),
        in_specs=[along, across, along, across, *cols, *cols, *rows, ANY],
        out_specs=[ANY] * 5 + [pl.BlockSpec((8, LANES), lambda c: (0, 0)), ANY],
        out_shape=[shape((tokens, ff))] * 2 + [shape((d // GROUP, ff))] * 2 + [shape((ff // GROUP, d)), shape((8, LANES), F32), shape(mine.shape, F32)],
        scratch_shapes=[VMEM((tokens, CHUNK), BF)] * 3 + [VMEM((d, CHUNK), BF)] * 2 + [VMEM((CHUNK, d), BF), DMA((2,)), DMA((2,))] + ring_scratch(d),
        compiler_params=params(1),
        name="layer1",
    )(a1, at1, dy, dyt, wg, wg, wu, wu, wd, wd, mine)


def input_kernel(dg_ref, du_ref, h_ref, dy_ref, wg_any, wu_any, d1_ref, dh_ref, dht_ref, all_ref, wg, wu, own, sem, *sems):
    step = pl.program_id(0)
    me, right, left, _ = around()
    bounce = sems[-1]
    to_stage = local(d1_ref.at[pl.ds(0, EARLY), :], own, bounce.at[0])
    from_stage = local(own, all_ref.at[span(me * EARLY, EARLY), :], bounce.at[1])
    near0, near1, far = spread(own, all_ref, *sems[:-1], EARLY)

    @pl.when(step == 0)
    def _():
        to_stage.start()
        copies = []
        for which, (src, dst) in enumerate(((wg_any, wg), (wu_any, wu))):
            for c in range(STEPS):
                for i, strip in enumerate((first_strip, second_strip)):
                    copies.append(local(src.at[1, :, span(LANES * strip(jnp.int32(c)), LANES, LANES)], dst.at[:, pl.ds(CHUNK * c + LANES * i, LANES)], sem.at[which, 2 * c + i]))
        start(copies)
        greet((right, left))
        to_stage.wait()
        start([*near0, *near1, from_stage])
        wait(copies)

    @pl.when(step == 4)
    def _():
        from_stage.wait()
        wait(near0)
        start(far)

    sub = TILE // 2

    def some(i, _):
        rows = span(i * sub, sub, sub)
        da = dot(dg_ref[rows, :], wg[ALL], NT).astype(BF).astype(F32) + dot(du_ref[rows, :], wu[ALL], NT).astype(BF).astype(F32)
        da = da.astype(BF).astype(F32)
        wide = h_ref[rows, :].astype(F32)
        _, scale = normed(wide)
        along = jnp.sum(da * wide, -1, keepdims=True) * (scale * scale * scale) / wide.shape[-1]
        back = (da * scale - wide * along).astype(BF)
        dh = (dy_ref[rows, :].astype(F32) + back.astype(F32)).astype(BF)
        dh_ref[rows, :] = dh
        dht_ref[:, rows] = dh.T

    lax.fori_loop(0, 2, some, None)

    @pl.when(step == pl.num_programs(0) - 1)
    def _():
        wait(near1 + far)


def input_gradient(dg, du, h, dy, wg, wu, d1):
    tokens, d = h.shape
    ff = dg.shape[1]
    row = pl.BlockSpec((TILE, d), lambda i: (i, 0))
    wide = pl.BlockSpec((TILE, ff), lambda i: (i, 0))
    return pl.pallas_call(
        input_kernel,
        grid=(tokens // TILE,),
        in_specs=[wide, wide, row, row, ANY, ANY, ANY],
        out_specs=[row, pl.BlockSpec((d, TILE), lambda i: (0, i)), ANY],
        out_shape=[shape((tokens, d)), shape((d, tokens)), shape((GROUP * EARLY, d))],
        scratch_shapes=[VMEM((d, ff), BF)] * 2 + [VMEM((EARLY, d), BF), DMA((2, 2 * STEPS))] + spread_scratch(),
        compiler_params=params(5),
        name="input1",
    )(dg, du, h, dy, wg, wu, d1)


def layer0_kernel(dh_ref, dht_ref, at_ref, g1, g2, u1, u2, wd1, wd2, g_out, u_out, d_out, sq_ref, act, dg, du, wd, *refs):
    c = pl.program_id(0)
    g, u, d = rings(refs, g_out, u_out, d_out)

    @pl.when(c == 0)
    def _():
        greet(around()[1:3])
        refs[-1][ALL] = jnp.zeros_like(refs[-1])

    wd[:LANES, :] = wd1[ALL]
    wd[LANES:, :] = wd2[ALL]

    def some(i, _):
        rows = span(i * TILE, TILE)
        dact_all = dot(dh_ref[rows, :], wd[ALL], NT).astype(BF).astype(F32)
        for j, (gate_ref, up_ref) in enumerate(((g1, u1), (g2, u2))):
            cols = slice(LANES * j, LANES * (j + 1))
            dact, gate, up = dact_all[:, cols], gate_ref[rows, :], up_ref[rows, :]
            s = jax.nn.sigmoid(gate)
            silu = gate * s
            act[rows, cols] = (silu * up).astype(BF)
            du[rows, cols] = (dact * silu).astype(BF)
            dg[rows, cols] = (dact * up * (s + silu * (1.0 - s))).astype(BF)

    lax.fori_loop(0, dh_ref.shape[0] // TILE, some, None)
    d.point(c)
    weight_gradients(c, at_ref, dht_ref, dg, du, act, refs, g, u, False)
    drain(c, refs, g, u, d, sq_ref)


def layer0(dh, dht, at0, gate, up, wd):
    tokens, d = dh.shape
    ff = gate.shape[1]
    along, across = (pl.BlockSpec(s, lambda c: (0, 0), pipeline_mode=ONE) for s in ((tokens, d), (d, tokens)))
    wide = [pl.BlockSpec((tokens, LANES), lambda c, s=s: (0, s(c))) for s in (first_strip, second_strip)]
    return pl.pallas_call(
        layer0_kernel,
        grid=(STEPS,),
        in_specs=[along, across, across, *wide, *wide, *strips_of(0, d)[1]],
        out_specs=[ANY] * 3 + [pl.BlockSpec((8, LANES), lambda c: (0, 0))],
        out_shape=[shape((d // GROUP, ff))] * 2 + [shape((ff // GROUP, d)), shape((8, LANES), F32)],
        scratch_shapes=[VMEM((tokens, CHUNK), BF)] * 3 + [VMEM((CHUNK, d), BF)] + ring_scratch(d),
        compiler_params=params(2),
        name="layer0",
    )(dh, dht, at0, gate, gate, up, up, wd, wd)


def moments_of(m, v, g):
    return 0.9 * m + 0.1 * g, 0.95 * v + 0.05 * g * g


def weight_of(w, m, v):
    return (w - 0.02 * (m * lax.rsqrt(v + 1e-8) + 0.1 * w)).astype(BF)


def gather_kernel(count, sq0, sq1, mg, vg, mu, vu, md, vd, wg, wu, wd, g0, g1, u0, u1, d0, d1, wg_all, wu_all, own, factor_ref, *scratch):
    (stage_g, stage_u, stage_d, m_up, v_up, w_up, g_up, m_dn, v_dn, w_dn, g_dn, sums, total, load, keep_sem, near_s, near_r, far_s, far_r, sum_s, sum_r, sum_l) = scratch
    me, right, left, across = around()
    pieces, rows = stage_g.shape[0], stage_g.shape[1]
    per = pieces // 2
    block = per * rows

    for other in (right, left, across):
        pl.semaphore_signal(pltpu.get_barrier_semaphore(), inc=1, device_id={"dp": other}, device_id_type=pl.DeviceIdType.MESH)
    pl.semaphore_wait(pltpu.get_barrier_semaphore(), HOPS)
    shares = [remote(sq, sums.at[n, j + 1], sum_s.at[n, j], sum_r.at[n, j], lax.rem(me + j + 1, GROUP)) for n, sq in enumerate((sq0, sq1)) for j in range(HOPS)]
    shares += [local(sq, sums.at[n, 0], sum_l.at[n]) for n, sq in enumerate((sq0, sq1))]
    start(shares)

    def loads(i, slot, arrays, gradient, bufs, layer, row, n, base):
        m, v, w = arrays
        here = span(row, n)
        sources = (m.at[layer, here, :], v.at[layer, here, :], w.at[layer, span(base + row, n), :], gradient.at[here, :])
        return [local(s, b.at[slot, pl.ds(0, n), :], load.at[j, slot]) for j, (s, b) in enumerate(zip(sources, bufs))]

    def update(slot, bufs, stage, i, n):
        m_buf, v_buf, w_buf, g_buf = bufs
        f = total[0:1, 0:1]

        def some(r, _):
            at = span(r * 16, 16)
            m, v = moments_of(m_buf[slot, at, :], v_buf[slot, at, :], g_buf[slot, at, :].astype(F32) * f)
            stage[i, at, :] = weight_of(w_buf[slot, at, :].astype(F32), m, v)

        lax.fori_loop(0, n // 16, some, None)

    def spot(dest, i, owner, at, n):
        return dest.at[lax.div(i, per), span(owner * block + lax.rem(i, per) * rows + at, n), :]

    def near(which, dest, stage, i, d):
        sems = near_s.at[which, i, d], near_r.at[which, i, d]
        return remote(stage.at[i], spot(dest, i, me, 0, rows), *sems, (right, left)[d])

    def far(which, dest, i, d):
        place = spot(dest, i, (left, right)[d], d * (rows // 2), rows // 2)
        return remote(place, place, far_s.at[which, i, d], far_r.at[which, i, d], (right, left)[d])

    def keep(which, dest, stage, i):
        return local(stage.at[i], spot(dest, i, me, 0, rows), keep_sem.at[which, i])

    up_bufs, down_bufs = (m_up, v_up, w_up, g_up), (m_dn, v_dn, w_dn, g_dn)
    ups = ((wg_all, stage_g, (mg, vg, wg), (g0, g1)), (wu_all, stage_u, (mu, vu, wu), (u0, u1)))

    def fetch(i, arrays, gradients):
        layer = lax.div(i, per)
        for n, gradient in enumerate(gradients):

            @pl.when(layer == n)
            def _():
                start(loads(i, lax.rem(i, 2), arrays, gradient, up_bufs, layer, lax.rem(i, per) * rows, rows, me * block))

    for which, (dest, stage, arrays, gradients) in enumerate(ups):
        fetch(jnp.int32(0), arrays, gradients)
        if which == 0:
            wait(shares)
            parts = [sums[0, lax.rem(me + GROUP - b, GROUP)] + sums[1, lax.rem(me + GROUP - b, GROUP)] for b in range(GROUP)]
            squares = jnp.sum(functools.reduce(jnp.add, parts), keepdims=True)
            factor = jnp.minimum(1.0, 0.5 * lax.rsqrt(squares / count + 1e-30))
            total[ALL] = jnp.broadcast_to(factor, total.shape)
            factor_ref[ALL] = jnp.broadcast_to(factor, total.shape)

        def body(i, _):
            slot = lax.rem(i, 2)

            @pl.when(i + 1 < pieces)
            def _():
                fetch(i + 1, arrays, gradients)

            wait(loads(i, slot, arrays, gradients[0], up_bufs, lax.div(i, per), lax.rem(i, per) * rows, rows, me * block))
            update(slot, up_bufs, stage, i, rows)
            start([keep(which, dest, stage, i), near(which, dest, stage, i, 0), near(which, dest, stage, i, 1)])

        lax.fori_loop(0, pieces, body, None)

    half = stage_d.shape[1]
    downs = [loads(0, n, (md, vd, wd), d0, down_bufs, 0, n * half, half, me * 2 * half) for n in range(2)]
    late = loads(0, 0, (md, vd, wd), d1, down_bufs, 1, EARLY, LATE, me * 2 * half)
    outs = [local(stage_d.at[n], own.at[pl.ds(n * half, half), :], sum_l.at[n]) for n in range(2)]
    outs.append(local(stage_d.at[2, pl.ds(0, LATE), :], own.at[pl.ds(2 * half, LATE), :], load.at[0, 1]))
    for copies in downs:
        start(copies)
    for n in range(2):
        wait(downs[n])
        update(n, down_bufs, stage_d, n, half)
        outs[n].start()
    start(late)
    wait(late)
    update(0, down_bufs, stage_d, 2, LATE)
    outs[2].start()

    for which, (dest, stage, _, _) in enumerate(ups):

        def onward(i, _):
            for d in range(2):
                near(which, dest, stage, i, d).wait()
                far(which, dest, i, d).start()

        lax.fori_loop(0, pieces, onward, None)
    for which, (dest, stage, _, _) in enumerate(ups):

        def finish(i, _):
            wait([keep(which, dest, stage, i), far(which, dest, i, 0), far(which, dest, i, 1)])

        lax.fori_loop(0, pieces, finish, None)
    wait(outs)


def gather(sq, moments, weights, gradients):
    mg, mu, md, vg, vu, vd = moments
    wg, wu, wd = weights
    _, d, ff = wg.shape
    pieces, rows, half = 2 * GROUP, d // GROUP // GROUP, ff // GROUP // 2
    up, down, each = (2, rows, ff), (2, half, d), (2, pieces, 2)
    return pl.pallas_call(
        functools.partial(gather_kernel, float(wg.size + wu.size + wd.size)),
        in_specs=[ANY] * 17,
        out_specs=[ANY] * 3 + [pl.BlockSpec(memory_space=VMEM)],
        out_shape=[shape(wg.shape), shape(wu.shape), shape((2 * half + LATE, d)), shape((8, LANES), F32)],
        scratch_shapes=[VMEM((pieces, rows, ff), BF)] * 2
        + [VMEM((3, half, d), BF)]
        + [VMEM(up, F32), VMEM(up, F32), VMEM(up, BF), VMEM(up, BF)]
        + [VMEM(down, F32), VMEM(down, F32), VMEM(down, BF), VMEM(down, BF)]
        + [VMEM((2, GROUP, 8, LANES), F32), VMEM((8, LANES), F32), DMA((4, 2)), DMA((2, pieces))]
        + [DMA(each)] * 4
        + [DMA((2, HOPS)), DMA((2, HOPS)), DMA((2,))],
        compiler_params=params(3),
        name="gather",
    )(*sq, mg, vg, mu, vu, md, vd, wg, wu, wd, *gradients)


def cost(args, outs):
    moved = sum(a.size * a.dtype.itemsize for a in (*args, *outs))
    return pl.CostEstimate(flops=moved * 300, bytes_accessed=moved, transcendentals=0)


def settle_moments(f, first, m, v, g0, g1, m_out, v_out):
    def some(r, _):
        at = span(r * 16, 16)
        g = jnp.where(first, g0[at, :].astype(F32), g1[at, :].astype(F32))
        m_out[0, at, :], v_out[0, at, :] = moments_of(m[0, at, :], v[0, at, :], g * f)

    lax.fori_loop(0, m.shape[1] // 16, some, None)


def moment_specs(rows, cols):
    part = pl.BlockSpec((1, rows // GROUP, cols), lambda i: (i // GROUP, i % GROUP, 0))
    one = pl.BlockSpec((rows // GROUP, cols), lambda i: (jnp.minimum(i, GROUP - 1), 0))
    two = pl.BlockSpec((rows // GROUP, cols), lambda i: (jnp.maximum(i - GROUP, 0), 0))
    return part, one, two


def settle_up_kernel(factor_ref, *refs):
    ins, outs = refs[:10], refs[10:]
    for n in range(2):
        m, v, g0, g1, w = ins[5 * n : 5 * n + 5]
        m_out, v_out, w_out = outs[3 * n : 3 * n + 3]
        settle_moments(factor_ref[0:1, 0:1], pl.program_id(0) < GROUP, m, v, g0, g1, m_out, v_out)
        w_out[ALL] = w[ALL]


def settle_up(factor, *args):
    _, rows, cols = args[0].shape
    part, one, two = moment_specs(rows, cols)
    whole = pl.BlockSpec((1, rows, cols), lambda i: (i // GROUP, i % GROUP, 0))
    outs = [shape(a.shape, a.dtype) for n in range(2) for a in (args[5 * n], args[5 * n + 1], args[5 * n + 4])]
    return pl.pallas_call(
        settle_up_kernel,
        grid=(2 * GROUP,),
        in_specs=[pl.BlockSpec((8, LANES), lambda i: (0, 0))] + [part, part, one, two, whole] * 2,
        out_specs=[part, part, whole] * 2,
        out_shape=outs,
        compiler_params=params(),
        cost_estimate=cost(args, outs),
        name="settle_up",
    )(factor, *args)


def settle_down_kernel(factor_ref, m, v, g0, g1, mine, other, g_all, w_any, m_out, v_out, w_out, w_buf, stage, load, store):
    i = pl.program_id(0)
    n = stage.shape[1]
    f = factor_ref[0:1, 0:1]

    def rows(k):
        return span(lax.div(k, 2) * (EARLY + LATE) + lax.rem(k, 2) * n, n)

    def into(k):
        return local(w_any.at[1, rows(k), :], w_buf.at[lax.rem(k, 2)], load.at[lax.rem(k, 2)])

    def out(k):
        return local(stage.at[lax.rem(k, 2)], w_out.at[1, rows(k), :], store.at[lax.rem(k, 2)])

    pl.when(i == 0)(lambda: into(i).start())
    pl.when(i + 1 < pl.num_programs(0))(lambda: into(i + 1).start())
    settle_moments(f, i < GROUP, m, v, g0, g1, m_out, v_out)
    pl.when(i > 1)(lambda: out(i - 2).wait())
    into(i).wait()
    even = lax.rem(lax.axis_index("rep"), 2) == 0
    slot = lax.rem(i, 2)

    def some(r, _):
        at = span(r * 16, 16)
        one, two = mine[at, :], other[at, :]
        new = moments_of(jnp.where(even, one, two), jnp.where(even, two, one), g_all[at, :].astype(F32) * f)
        stage[slot, at, :] = weight_of(w_buf[slot, at, :].astype(F32), *new)

    lax.fori_loop(0, n // 16, some, None)
    out(i).start()

    @pl.when(i == pl.num_programs(0) - 1)
    def _():
        wait([out(i - 1), out(i)])


def settle_down(factor, m, v, g0, g1, mine, other, g_all, w):
    _, rows, cols = m.shape
    part, one, two = moment_specs(rows, cols)
    tile = EARLY // 2
    early = pl.BlockSpec((tile, cols), lambda i: (i, 0))
    outs = [shape(m.shape, F32), shape(v.shape, F32), shape(w.shape)]
    args = (m, v, g0, g1, mine, other, g_all)
    return pl.pallas_call(
        settle_down_kernel,
        grid=(2 * GROUP,),
        in_specs=[pl.BlockSpec((8, LANES), lambda i: (0, 0)), part, part, one, two, early, early, early, ANY],
        out_specs=[part, part, ANY],
        out_shape=outs,
        scratch_shapes=[VMEM((2, tile, cols), BF)] * 2 + [DMA((2,))] * 2,
        compiler_params=params(),
        cost_estimate=cost(args, outs),
        name="settle_down",
    )(factor, *args, w)


def place_kernel(own, from_left, from_right, head, tail, _, out, sem):
    me, right, left, across = around()
    block = EARLY + LATE
    half = head.shape[0]
    copies = []

    def put(src, layer, at, n):
        copies.append(local(src, out.at[layer, span(at, n), :], sem.at[len(copies)]))

    for src, owner in ((own, me), (from_left, left), (from_right, right)):
        put(src.at[pl.ds(0, block), :], 0, owner * block, block)
        put(src.at[pl.ds(block, LATE), :], 1, owner * block + EARLY, LATE)
    put(head, 0, across * block, half)
    put(tail.at[pl.ds(0, block - half), :], 0, across * block + half, block - half)
    put(tail.at[pl.ds(block - half, LATE), :], 1, across * block + EARLY, LATE)
    start(copies)
    wait(copies)


def place(blocks, out):
    return pl.pallas_call(
        place_kernel,
        in_specs=[pl.BlockSpec(memory_space=VMEM)] * len(blocks) + [ANY],
        out_specs=ANY,
        out_shape=shape(out.shape),
        scratch_shapes=[DMA((9,))],
        input_output_aliases={len(blocks): 0},
        compiler_params=params(),
        name="place",
    )(*blocks, out)


def solution(mesh):
    def step(x, dy, wg, wu, wd, mg, mu, md, vg, vu, vd):
        x, dy = x[0], dy[0]
        gate, up, at0, h, a1, at1, dyt, mine = forward(x, dy, wg, wu, wd, md, vd)
        dgate, dup, g1, u1, d1, sq1, other = layer1(a1, at1, dy, dyt, wg, wu, wd, mine)
        dh, dht, d1_all = input_gradient(dgate, dup, h, dy, wg, wu, d1)
        g0, u0, d0, sq0 = layer0(dh, dht, at0, gate, up, wd)
        all_g, all_u, own, factor = gather((sq0, sq1), (mg, mu, md, vg, vu, vd), (wg, wu, wd), (g0, g1, u0, u1, d0, d1))
        to_right, to_left = ([(i, (i + away) % GROUP) for i in range(GROUP)] for away in (1, HOPS))
        half = own.shape[0] // 2
        from_left, from_right = lax.ppermute(own, "dp", to_right), lax.ppermute(own, "dp", to_left)
        mg, vg, new_g, mu, vu, new_u = settle_up(factor, mg, vg, g0, g1, all_g, mu, vu, u0, u1, all_u)
        from_left, from_right, new_g, factor = lax.optimization_barrier((from_left, from_right, new_g, factor))
        head, tail = lax.ppermute(from_left[:half], "dp", to_right), lax.ppermute(from_right[half:], "dp", to_left)
        md, vd, new_d = settle_down(factor, md, vd, d0, d1, mine, other, d1_all, wd)
        new_d = place((own, from_left, from_right, head, tail), new_d)
        return new_g, new_u, new_d, mg, mu, md, vg, vu, vd

    whole, part = P(), P(None, "dp", None)
    return jax.shard_map(
        step,
        mesh=mesh,
        in_specs=(P(("rep", "dp")),) * 2 + (whole,) * 3 + (part,) * 6,
        out_specs=(P("rep"),) * 3 + (P("rep", "dp", None),) * 6,
        check_vma=False,
    )
```

```python
import functools

import jax
import jax.numpy as jnp
from jax import lax
from jax.experimental import pallas as pl
from jax.experimental.pallas import tpu as pltpu
from jax.sharding import PartitionSpec as P

BF = jnp.bfloat16
F32 = jnp.float32
VMEM = pltpu.VMEM
DMA = pltpu.SemaphoreType.DMA
NN = (((1,), (0,)), ((), ()))
NT = (((1,), (1,)), ((), ()))
ONE = pl.Buffered(1)
ANY = pl.BlockSpec(memory_space=pl.ANY)
ALL = ...
LANES = 128
CHUNK = 256
STEPS = 11
LAST = STEPS - 1
TILE = 512
GROUP = 4
HOPS = GROUP - 1
EARLY = 576
LATE = 128


def shape(dims, dtype=BF):
    return jax.ShapeDtypeStruct(dims, dtype)


def params(collective_id=None):
    limit = 67_000_000
    if collective_id is None:
        return pltpu.CompilerParams(vmem_limit_bytes=limit)
    return pltpu.CompilerParams(vmem_limit_bytes=limit, collective_id=collective_id, has_side_effects=True)


def dot(a, b, dims):
    return lax.dot_general(a, b, dims, preferred_element_type=F32)


def span(start, size, multiple=16):
    return pl.ds(pl.multiple_of(start, multiple), size)


def local(src, dst, sem):
    return pltpu.make_async_copy(src, dst, sem)


def remote(src, dst, sent, received, to, axis="dp"):
    return pltpu.make_async_remote_copy(
        src_ref=src, dst_ref=dst, send_sem=sent, recv_sem=received, device_id={axis: to}, device_id_type=pl.DeviceIdType.MESH
    )


def around():
    me = lax.axis_index("dp")
    return (me, *(lax.rem(me + away, GROUP) for away in (1, HOPS, 2)))


def partner():
    rep = lax.axis_index("rep")
    return rep + 1 - 2 * lax.rem(rep, 2)


def greet(devices, groups=()):
    barrier = pltpu.get_barrier_semaphore()
    for axis, others in (("dp", devices), ("rep", groups)):
        for other in others:
            pl.semaphore_signal(barrier, inc=1, device_id={axis: other}, device_id_type=pl.DeviceIdType.MESH)
    pl.semaphore_wait(barrier, len(devices) + len(groups))


def start(copies):
    for c in copies:
        c.start()


def wait(copies):
    for c in copies:
        c.wait()


def first_strip(c):
    return jnp.where(c == LAST, 5, jnp.where(c % 2 == 0, c // 2, STEPS + c // 2))


def second_strip(c):
    return jnp.where(c == LAST, 16, jnp.where(c % 2 == 0, c // 2 + 6, c // 2 + 17))


def normed(wide):
    scale = lax.rsqrt(jnp.mean(wide * wide, -1, keepdims=True) + 1e-6)
    return (wide * scale).astype(BF), scale


def spread(source, dest, near_s, near_r, far_s, far_r, rows):
    me, right, left, _ = around()
    half = rows // 2
    to = (right, left)

    def near(d, n):
        part = n if d == 0 else 1 - n
        return remote(source.at[span(part * half, half), :], dest.at[span(me * rows + part * half, half), :], near_s.at[d, n], near_r.at[d, n], to[d])

    def far(d):
        spot = dest.at[span((left, right)[d] * rows + d * half, half), :]
        return remote(spot, spot, far_s.at[d], far_r.at[d], to[d])

    ways = range(2)
    return [near(d, 0) for d in ways], [near(d, 1) for d in ways], [far(d) for d in ways]


def spread_scratch():
    return [DMA((2, 2)), DMA((2, 2)), DMA((2,)), DMA((2,)), DMA((2,))]


def forward_kernel(x_ref, dy_ref, wg_ref, wu_ref, wd_ref, m_ref, v_ref, gate_ref, up_ref, at0_ref, h_ref, a1_ref, at1_ref, dyt_ref, mine_ref, act, moment, *sems):
    step = pl.program_id(0)
    me, right, left, _ = around()
    kind = lax.rem(lax.axis_index("rep"), 2)
    bounce = sems[-1]
    to_stage = [local(ref.at[1, pl.ds(0, EARLY), :], moment, bounce.at[0]) for ref in (m_ref, v_ref)]
    from_stage = local(moment, mine_ref.at[span(me * EARLY, EARLY), :], bounce.at[1])
    near0, near1, far = spread(moment, mine_ref, *sems[:-1], EARLY)

    @pl.when(step == 0)
    def _():
        for n, copy in enumerate(to_stage):
            pl.when(kind == n)(copy.start)
        greet((right, left))
        to_stage[0].wait()
        start(near0 + near1 + [from_stage])

    @pl.when(step == 5)
    def _():
        from_stage.wait()
        wait(near0)
        start(far)

    dyt_ref[ALL] = dy_ref[ALL].T
    sub = TILE // 2
    for i in range(2):
        rows = slice(i * sub, (i + 1) * sub)
        a, _ = normed(x_ref[rows, :].astype(F32))
        at0_ref[:, rows] = a.T
        for c in range(STEPS):
            cols = slice(CHUNK * c, CHUNK * (c + 1))
            gate = dot(a, wg_ref[:, cols], NN)
            up = dot(a, wu_ref[:, cols], NN)
            gate_ref[rows, cols] = gate
            up_ref[rows, cols] = up
            act[rows, cols] = (gate * jax.nn.sigmoid(gate) * up).astype(BF)
    for i in range(2):
        rows = slice(i * sub, (i + 1) * sub)
        down = dot(act[rows, :], wd_ref[ALL], NN).astype(BF)
        h = (x_ref[rows, :].astype(F32) + down.astype(F32)).astype(BF)
        h_ref[rows, :] = h
        a1, _ = normed(h.astype(F32))
        a1_ref[rows, :] = a1
        at1_ref[:, rows] = a1.T

    @pl.when(step == pl.num_programs(0) - 1)
    def _():
        wait(near1 + far)


def forward(x, dy, wg, wu, wd, m, v):
    tokens, d = x.shape
    ff = wg.shape[2]
    row = pl.BlockSpec((TILE, d), lambda i: (i, 0))
    col = pl.BlockSpec((d, TILE), lambda i: (0, i))
    wide = pl.BlockSpec((TILE, ff), lambda i: (i, 0))
    up_spec = pl.BlockSpec((None, d, ff), lambda i: (0, 0, 0), pipeline_mode=ONE)
    down_spec = pl.BlockSpec((None, ff, d), lambda i: (0, 0, 0), pipeline_mode=ONE)
    across, along = shape((d, tokens)), shape((tokens, d))
    return pl.pallas_call(
        forward_kernel,
        grid=(tokens // TILE,),
        in_specs=[row, row, up_spec, up_spec, down_spec, ANY, ANY],
        out_specs=[wide, wide, col, row, row, col, col, ANY],
        out_shape=[shape((tokens, ff), F32)] * 2 + [across, along, along, across, across, shape((GROUP * EARLY, d), F32)],
        scratch_shapes=[VMEM((TILE, ff), BF), VMEM((EARLY, d), F32)] + spread_scratch(),
        compiler_params=params(4),
        name="fwd0",
    )(x, dy, wg, wu, wd, m, v)


class Ring:
    def __init__(self, item, rows, refs, emit):
        self.item = item
        self.rows = rows
        self.term, self.recv, self.send, self.fin, self.ssem, self.rsem, self.total = refs
        self.emit = emit

    def mine(self, h, d, k, half, away):
        me = lax.axis_index("dp")
        away = away + h
        block = lax.rem(me + 2 * GROUP - away, GROUP) if d == 0 else lax.rem(me + away, GROUP)
        return lax.rem(k, self.term.shape[0]), span(block * 2 * half + d * half, half, half), slice(None)

    def copy(self, h, d, k, half):
        _, right, left, _ = around()
        spot = (d, lax.rem(k, 2), pl.ds(0, half), slice(None))
        src = self.term.at[self.mine(h, d, k, half, 1)] if h == 0 else self.send.at[h - 1, *spot]
        sems = self.ssem.at[h, *spot[:2]], self.rsem.at[h, *spot[:2]]
        return remote(src, self.recv.at[h, *spot], *sems, (right, left)[d])

    def each(self, t, body):
        there, k = self.item(t)
        for condition, half in self.rows:
            where = there if condition is None else jnp.logical_and(there, condition(k))
            pl.when(where)(functools.partial(body, k, half))

    def point(self, t):
        ways = range(2)

        def arrived(h, k, half):
            wait([self.copy(h, d, k, half) for d in ways])

        def add(h, k, half):
            slot = lax.rem(k, 2)
            for d in ways:
                spot = (d, slot, pl.ds(0, half), slice(None))
                value = (self.recv[h, *spot].astype(F32) + self.term[self.mine(h, d, k, half, 2)].astype(F32)).astype(BF)
                if h < HOPS - 1:
                    self.send[h, *spot] = value
                else:
                    self.fin[slot, pl.ds(d * half, half), :] = value
                    square = value.astype(F32) ** 2
                    parts = [square[:, LANES * i : LANES * (i + 1)] for i in range(square.shape[1] // LANES)]
                    self.total[ALL] += jnp.sum(functools.reduce(jnp.add, parts).reshape(half // 8, 8, LANES), 0)

        def leave(h, k, half):
            start([self.copy(h, d, k, half) for d in ways])

        def out(k, half):
            start(self.emit(k, lax.rem(k, 2), 2 * half))

        def gone(k, half):
            wait(self.emit(k, lax.rem(k, 2), 2 * half))

        for h in range(HOPS):
            self.each(t - 1 - h, functools.partial(arrived, h))
        self.each(t - HOPS - 1, gone)
        for h in range(HOPS):
            self.each(t - 1 - h, functools.partial(add, h))
        for h in range(HOPS):
            self.each(t - h, functools.partial(leave, h))
        self.each(t - HOPS, out)


def rings(refs, g_out, u_out, d_out):
    (g_term, u_term, d_term, g_recv, u_recv, d_recv, g_send, u_send, d_send, g_fin, u_fin, d_fin, ssem, rsem, fsem, total) = refs
    me = lax.axis_index("dp")

    def every(t):
        return jnp.logical_and(t >= 0, t < STEPS), t

    def pairs(t):
        last = t == STEPS
        return jnp.logical_or(last, jnp.logical_and(jnp.logical_and(t >= 2, t < STEPS), lax.rem(t, 2) == 0)), jnp.where(last, 5, lax.div(t, 2) - 1)

    def columns(fin, out, sem):
        def emit(k, slot, rows):
            return [
                local(fin.at[slot, :, pl.ds(LANES * i, LANES)], out.at[:, span(LANES * strip(k), LANES, LANES)], sem.at[slot, i])
                for i, strip in enumerate((first_strip, second_strip))
            ]

        return emit

    def down(k, slot, rows):
        odd = lax.rem(me, 2)
        at = LANES * k + 64 * odd if rows == LANES else 640 * (1 - odd)
        return [local(d_fin.at[slot, pl.ds(0, rows), :], d_out.at[span(at, rows, 64), :], fsem.at[2, slot, 0])]

    halves = [(None, LANES)]
    return (
        Ring(every, halves, (g_term, g_recv, g_send, g_fin, ssem.at[0], rsem.at[0], total), columns(g_fin, g_out, fsem.at[0])),
        Ring(every, halves, (u_term, u_recv, u_send, u_fin, ssem.at[1], rsem.at[1], total), columns(u_fin, u_out, fsem.at[1])),
        Ring(pairs, [(lambda k: k < 5, 64), (lambda k: k == 5, 32)], (d_term, d_recv, d_send, d_fin, ssem.at[2], rsem.at[2], total), down),
    )


def ring_scratch(d):
    up, down = (2, 2, LANES, CHUNK), (2, 2, 64, d)
    return (
        [VMEM((GROUP, d, CHUNK), BF)] * 2
        + [VMEM((3, TILE, d), BF)]
        + [VMEM((HOPS, *up), BF)] * 2
        + [VMEM((HOPS, *down), BF)]
        + [VMEM((HOPS - 1, *up), BF)] * 2
        + [VMEM((HOPS - 1, *down), BF)]
        + [VMEM((2, CHUNK, CHUNK), BF)] * 2
        + [VMEM((2, LANES, d), BF), DMA((3, HOPS, 2, 2)), DMA((3, HOPS, 2, 2)), DMA((3, 2, 2)), VMEM((8, LANES), F32)]
    )


def weight_gradients(c, at_ref, dyt_ref, dg, du, act, refs, g, u):
    half = at_ref.shape[0] // 2
    halves = [slice(0, half), slice(half, 2 * half)]
    for term, right in zip(refs[:2], (dg, du)):
        for rows in halves:
            term[lax.rem(c, GROUP), rows, :] = dot(at_ref[rows, :], right[ALL], NN).astype(BF)
    g.point(c)
    for rows in halves:
        value = dot(dyt_ref[rows, :], act[ALL], NN).astype(BF).T
        refs[2][lax.rem(c // 2, 3), span(CHUNK * lax.rem(c, 2), CHUNK), rows] = value
    u.point(c)


def gated(gate, up, dact):
    s = jax.nn.sigmoid(gate)
    silu = gate * s
    return (silu * up).astype(BF), (dact * silu).astype(BF), (dact * up * (s + silu * (1.0 - s))).astype(BF)


def strips(c):
    return first_strip(c), second_strip(c)


def columns_in(src, dst, sem, c):
    return [local(src.at[:, span(LANES * k, LANES, LANES)], dst.at[:, pl.ds(LANES * i, LANES)], sem.at[i]) for i, k in enumerate(strips(c))]


def rows_in(src, dst, sem, c):
    return [local(src.at[span(LANES * k, LANES), :], dst.at[pl.ds(LANES * i, LANES), :], sem.at[i]) for i, k in enumerate(strips(c))]


def backward_kernel(a_any, at1_any, dy_any, dyt_any, at0_any, gate_any, up_any, h_any, wg_any, wu_any, wd_any, mine_ref, dgate_out, dup_out, g1, u1, d1, g0, u0, d0, other_ref, early_ref, sq_ref, own, osem, msem, wsem, *scratch):
    refs, sems = scratch[:16], scratch[16:]
    me, right, left, _ = around()
    tokens, width = a_any.shape
    tiles = tokens // TILE
    exchange = remote(mine_ref, other_ref, msem.at[0], msem.at[1], partner(), "rep")

    def layer1(a_ref, at_ref, dy_ref, dyt_ref, act, dg, du, wg, wu, wd, tile_sem, whole_sem):
        g, u, d = rings(refs, g1, u1, d1)

        def weights(c):
            slot = lax.rem(c, 2)
            return (
                columns_in(wg_any.at[1], wg.at[slot], wsem.at[0, slot], c)
                + columns_in(wu_any.at[1], wu.at[slot], wsem.at[1, slot], c)
                + rows_in(wd_any.at[1], wd.at[slot], wsem.at[2, slot], c)
            )

        def arrive(i):
            rows = span(TILE * i, TILE)
            return [local(src.at[rows, :], dst.at[rows, :], tile_sem.at[n, i]) for n, (src, dst) in enumerate(((a_any, a_ref), (dy_any, dy_ref)))]

        whole = [local(at1_any, at_ref, whole_sem.at[0]), local(dyt_any, dyt_ref, whole_sem.at[1])]

        def put(k):
            cols = span(CHUNK * k, CHUNK, CHUNK)
            return [local(dg, dgate_out.at[:, cols], osem.at[0]), local(du, dup_out.at[:, cols], osem.at[1])]

        start(weights(jnp.int32(0)))
        for i in range(tiles):
            start(arrive(i))
        start(whole)
        refs[-1][ALL] = jnp.zeros_like(refs[-1])
        greet((right, left), (partner(),))

        def chunk(c, _):
            slot = lax.rem(c, 2)
            pl.when(c < LAST)(lambda: start(weights(c + 1)))
            pl.when(c > 0)(lambda: wait(put(c - 1)))
            pl.when(c == 2)(exchange.start)
            wait(weights(c))

            def some(rows):
                gate = dot(a_ref[rows, :], wg[slot], NN)
                up = dot(a_ref[rows, :], wu[slot], NN)
                dact = dot(dy_ref[rows, :], wd[slot], NT).astype(BF).astype(F32)
                act[rows, :], du[rows, :], dg[rows, :] = gated(gate, up, dact)

            @pl.when(c == 0)
            def _():
                def one(i, _):
                    wait(arrive(i))
                    some(span(TILE * i, TILE))

                lax.fori_loop(0, tiles, one, None)
                wait(whole)

            @pl.when(c > 0)
            def _():
                for i in range(tiles):
                    some(slice(TILE * i, TILE * (i + 1)))

            d.point(c)
            start(put(c))
            weight_gradients(c, at_ref, dyt_ref, dg, du, act, refs, g, u)

        lax.fori_loop(0, STEPS, chunk, None)
        wait(put(LAST))

    def input_gradient(dh_ref, dht_ref, wg, wu, dg_buf, du_buf, h_buf, dy_buf, sem, tile_sem):
        g, u, d = rings(refs, g1, u1, d1)
        n = dg_buf.shape[1]

        def tile(j):
            slot = lax.rem(j, 2)
            rows = span(n * j, n)
            pairs = ((dgate_out, dg_buf), (dup_out, du_buf), (h_any, h_buf), (dy_any, dy_buf))
            return [local(src.at[rows, :], dst.at[slot], tile_sem.at[i, slot]) for i, (src, dst) in enumerate(pairs)]

        start(tile(jnp.int32(0)))
        copies = [columns_in(src.at[1], dst.at[:, pl.ds(CHUNK * c, CHUNK)], sem.at[i, c], jnp.int32(c)) for i, (src, dst) in enumerate(((wg_any, wg), (wu_any, wu))) for c in range(STEPS)]
        start(sum(copies, []))
        wait(sum(copies, []))
        bounce = sems[-1]
        to_stage = local(d1.at[pl.ds(0, EARLY), :], own, bounce.at[0])
        from_stage = local(own, early_ref.at[span(me * EARLY, EARLY), :], bounce.at[1])
        near0, near1, far = spread(own, early_ref, *sems[:-1], EARLY)

        def one(j, _):
            slot = lax.rem(j, 2)
            pl.when(j + 1 < tokens // n)(lambda: start(tile(j + 1)))

            @pl.when(jnp.logical_and(j > 0, j < HOPS + 3))
            def _():
                for ring in (d, g, u):
                    ring.point(j + LAST)

            @pl.when(j == HOPS + 2)
            def _():
                to_stage.start()
                to_stage.wait()
                start([*near0, *near1, from_stage])

            @pl.when(j == 10)
            def _():
                from_stage.wait()
                wait(near0)
                start(far)

            wait(tile(j))
            da = dot(dg_buf[slot], wg[ALL], NT).astype(BF).astype(F32) + dot(du_buf[slot], wu[ALL], NT).astype(BF).astype(F32)
            da = da.astype(BF).astype(F32)
            wide = h_buf[slot].astype(F32)
            _, scale = normed(wide)
            along = jnp.sum(da * wide, -1, keepdims=True) * (scale * scale * scale) / width
            back = (da * scale - wide * along).astype(BF)
            dh = (dy_buf[slot].astype(F32) + back.astype(F32)).astype(BF)
            rows = span(n * j, n, n)
            dh_ref[rows, :] = dh
            dht_ref[:, rows] = dh.T

        lax.fori_loop(0, tokens // n, one, None)
        wait(near1 + far)

    def layer0(dh_ref, dht_ref, at_ref, gate_buf, up_buf, act, dg, du, wd, tile_sem):
        g, u, d = rings(refs, g0, u0, d0)

        def weights(c):
            slot = lax.rem(c, 2)
            return rows_in(wd_any.at[0], wd.at[slot], wsem.at[2, slot], c)

        def arrive(c, i):
            slot = lax.rem(c, 2)
            rows = span(TILE * i, TILE)
            return [copy for n, (src, dst) in enumerate(((gate_any, gate_buf), (up_any, up_buf))) for copy in columns_in(src.at[rows, :], dst.at[slot, rows, :], tile_sem.at[slot, i, n], c)]

        def fetch(c):
            start(weights(c))
            lax.fori_loop(0, tiles, lambda i, _: start(arrive(c, i)), None)

        fetch(jnp.int32(0))

        def chunk(c, _):
            slot = lax.rem(c, 2)
            pl.when(c < LAST)(lambda: fetch(c + 1))
            wait(weights(c))

            def some(i, _):
                rows = span(TILE * i, TILE)
                wait(arrive(c, i))
                dact = dot(dh_ref[rows, :], wd[slot], NT).astype(BF).astype(F32)
                act[rows, :], du[rows, :], dg[rows, :] = gated(gate_buf[slot, rows, :], up_buf[slot, rows, :], dact)

            lax.fori_loop(0, tiles, some, None)
            d.point(c)
            weight_gradients(c, at_ref, dht_ref, dg, du, act, refs, g, u)

        lax.fori_loop(0, STEPS, chunk, None)

        def drain(t, _):
            for ring in (d, g, u):
                ring.point(t)

        lax.fori_loop(STEPS, STEPS + HOPS + 2, drain, None)

    along, across = VMEM((tokens, width), BF), VMEM((width, tokens), BF)
    parts = [VMEM((tokens, CHUNK), BF)] * 3
    up_strip, down_strip = VMEM((2, width, CHUNK), BF), VMEM((2, CHUNK, width), BF)
    pl.run_scoped(layer1, along, across, along, across, *parts, up_strip, up_strip, down_strip, DMA((2, tiles)), DMA((2,)))

    def rest(dh_ref, dht_ref, at_ref, at_sem):
        ff = dgate_out.shape[1]
        fetched = local(at0_any, at_ref, at_sem.at[0])
        fetched.start()
        n = TILE // 2
        whole, wide, narrow = VMEM((width, ff), BF), VMEM((2, n, ff), BF), VMEM((2, n, width), BF)
        pl.run_scoped(functools.partial(input_gradient, dh_ref, dht_ref), whole, whole, wide, wide, narrow, narrow, DMA((2, STEPS, 2)), DMA((4, 2)))
        fetched.wait()
        strip = VMEM((2, tokens, CHUNK), F32)
        pl.run_scoped(functools.partial(layer0, dh_ref, dht_ref, at_ref), strip, strip, *parts, down_strip, DMA((2, tiles, 2, 2)))

    pl.run_scoped(rest, along, across, across, DMA((1,)))
    exchange.wait()
    sq_ref[ALL] = refs[-1][ALL]


def backward(a1, at1, dy, dyt, at0, gate, up, h, wg, wu, wd, mine):
    tokens, d = a1.shape
    ff = wg.shape[2]
    wide, block_up, block_down = shape((tokens, ff)), shape((d // GROUP, ff)), shape((ff // GROUP, d))
    return pl.pallas_call(
        backward_kernel,
        in_specs=[ANY] * 12,
        out_specs=[ANY] * 10 + [pl.BlockSpec(memory_space=VMEM)],
        out_shape=[wide, wide] + [block_up, block_up, block_down] * 2 + [shape(mine.shape, F32), shape(mine.shape), shape((8, LANES), F32)],
        scratch_shapes=[VMEM((EARLY, d), BF), DMA((2,)), DMA((2,)), DMA((3, 2, 2))] + ring_scratch(d) + spread_scratch(),
        compiler_params=params(1),
        name="backward",
    )(a1, at1, dy, dyt, at0, gate, up, h, wg, wu, wd, mine)


def moments_of(m, v, g):
    return 0.9 * m + 0.1 * g, 0.95 * v + 0.05 * g * g


def weight_of(w, m, v):
    return (w - 0.02 * (m * lax.rsqrt(v + 1e-8) + 0.1 * w)).astype(BF)


def gather_kernel(count, sq, mg, vg, mu, vu, md, vd, wg, wu, wd, g0, g1, u0, u1, d0, d1, wg_all, wu_all, own, factor_ref, *scratch):
    (stage_g, stage_u, stage_d, m_up, v_up, w_up, g_up, m_dn, v_dn, w_dn, g_dn, sums, total, load, keep_sem, near_s, near_r, far_s, far_r, sum_s, sum_r, sum_l) = scratch
    me, right, left, across = around()
    pieces, rows = stage_g.shape[0], stage_g.shape[1]
    per = pieces // 2
    block = per * rows

    for other in (right, left, across):
        pl.semaphore_signal(pltpu.get_barrier_semaphore(), inc=1, device_id={"dp": other}, device_id_type=pl.DeviceIdType.MESH)
    pl.semaphore_wait(pltpu.get_barrier_semaphore(), HOPS)
    shares = [remote(sq, sums.at[j + 1], sum_s.at[j], sum_r.at[j], lax.rem(me + j + 1, GROUP)) for j in range(HOPS)]
    shares.append(local(sq, sums.at[0], sum_l.at[0]))
    start(shares)

    def loads(i, slot, arrays, gradient, bufs, layer, row, n, base):
        m, v, w = arrays
        here = span(row, n)
        sources = (m.at[layer, here, :], v.at[layer, here, :], w.at[layer, span(base + row, n), :], gradient.at[here, :])
        return [local(s, b.at[slot, pl.ds(0, n), :], load.at[j, slot]) for j, (s, b) in enumerate(zip(sources, bufs))]

    def update(slot, bufs, stage, i, n):
        m_buf, v_buf, w_buf, g_buf = bufs
        f = total[0:1, 0:1]

        def some(r, _):
            at = span(r * 16, 16)
            m, v = moments_of(m_buf[slot, at, :], v_buf[slot, at, :], g_buf[slot, at, :].astype(F32) * f)
            stage[i, at, :] = weight_of(w_buf[slot, at, :].astype(F32), m, v)

        lax.fori_loop(0, n // 16, some, None)

    def spot(dest, i, owner, at, n):
        return dest.at[lax.div(i, per), span(owner * block + lax.rem(i, per) * rows + at, n), :]

    def near(which, dest, stage, i, d):
        sems = near_s.at[which, i, d], near_r.at[which, i, d]
        return remote(stage.at[i], spot(dest, i, me, 0, rows), *sems, (right, left)[d])

    def far(which, dest, i, d):
        place = spot(dest, i, (left, right)[d], d * (rows // 2), rows // 2)
        return remote(place, place, far_s.at[which, i, d], far_r.at[which, i, d], (right, left)[d])

    def keep(which, dest, stage, i):
        return local(stage.at[i], spot(dest, i, me, 0, rows), keep_sem.at[which, i])

    up_bufs, down_bufs = (m_up, v_up, w_up, g_up), (m_dn, v_dn, w_dn, g_dn)
    ups = ((wg_all, stage_g, (mg, vg, wg), (g0, g1)), (wu_all, stage_u, (mu, vu, wu), (u0, u1)))

    def fetch(i, arrays, gradients):
        layer = lax.div(i, per)
        for n, gradient in enumerate(gradients):

            @pl.when(layer == n)
            def _():
                start(loads(i, lax.rem(i, 2), arrays, gradient, up_bufs, layer, lax.rem(i, per) * rows, rows, me * block))

    for which, (dest, stage, arrays, gradients) in enumerate(ups):
        fetch(jnp.int32(0), arrays, gradients)
        if which == 0:
            wait(shares)
            parts = [sums[lax.rem(me + GROUP - b, GROUP)] for b in range(GROUP)]
            squares = jnp.sum(functools.reduce(jnp.add, parts), keepdims=True)
            factor = jnp.minimum(1.0, 0.5 * lax.rsqrt(squares / count + 1e-30))
            total[ALL] = jnp.broadcast_to(factor, total.shape)
            factor_ref[ALL] = jnp.broadcast_to(factor, total.shape)

        def body(i, _):
            slot = lax.rem(i, 2)

            @pl.when(i + 1 < pieces)
            def _():
                fetch(i + 1, arrays, gradients)

            wait(loads(i, slot, arrays, gradients[0], up_bufs, lax.div(i, per), lax.rem(i, per) * rows, rows, me * block))
            update(slot, up_bufs, stage, i, rows)
            start([keep(which, dest, stage, i), near(which, dest, stage, i, 0), near(which, dest, stage, i, 1)])

        lax.fori_loop(0, pieces, body, None)

    half = stage_d.shape[1]
    downs = [loads(0, n, (md, vd, wd), d0, down_bufs, 0, n * half, half, me * 2 * half) for n in range(2)]
    late = loads(0, 0, (md, vd, wd), d1, down_bufs, 1, EARLY, LATE, me * 2 * half)
    outs = [local(stage_d.at[n], own.at[pl.ds(n * half, half), :], sum_l.at[n]) for n in range(2)]
    outs.append(local(stage_d.at[2, pl.ds(0, LATE), :], own.at[pl.ds(2 * half, LATE), :], load.at[0, 1]))
    for copies in downs:
        start(copies)
    for n in range(2):
        wait(downs[n])
        update(n, down_bufs, stage_d, n, half)
        outs[n].start()
    start(late)
    wait(late)
    update(0, down_bufs, stage_d, 2, LATE)
    outs[2].start()

    for which, (dest, stage, _, _) in enumerate(ups):

        def onward(i, _):
            for d in range(2):
                near(which, dest, stage, i, d).wait()
                far(which, dest, i, d).start()

        lax.fori_loop(0, pieces, onward, None)
    for which, (dest, stage, _, _) in enumerate(ups):

        def finish(i, _):
            wait([keep(which, dest, stage, i), far(which, dest, i, 0), far(which, dest, i, 1)])

        lax.fori_loop(0, pieces, finish, None)
    wait(outs)


def gather(sq, moments, weights, gradients):
    mg, mu, md, vg, vu, vd = moments
    wg, wu, wd = weights
    _, d, ff = wg.shape
    pieces, rows, half = 2 * GROUP, d // GROUP // GROUP, ff // GROUP // 2
    up, down, each = (2, rows, ff), (2, half, d), (2, pieces, 2)
    return pl.pallas_call(
        functools.partial(gather_kernel, float(wg.size + wu.size + wd.size)),
        in_specs=[ANY] * 16,
        out_specs=[ANY] * 3 + [pl.BlockSpec(memory_space=VMEM)],
        out_shape=[shape(wg.shape), shape(wu.shape), shape((2 * half + LATE, d)), shape((8, LANES), F32)],
        scratch_shapes=[VMEM((pieces, rows, ff), BF)] * 2
        + [VMEM((3, half, d), BF)]
        + [VMEM(up, F32), VMEM(up, F32), VMEM(up, BF), VMEM(up, BF)]
        + [VMEM(down, F32), VMEM(down, F32), VMEM(down, BF), VMEM(down, BF)]
        + [VMEM((GROUP, 8, LANES), F32), VMEM((8, LANES), F32), DMA((4, 2)), DMA((2, pieces))]
        + [DMA(each)] * 4
        + [DMA((HOPS,)), DMA((HOPS,)), DMA((2,))],
        compiler_params=params(3),
        name="gather",
    )(sq, mg, vg, mu, vu, md, vd, wg, wu, wd, *gradients)


def cost(args, outs):
    moved = sum(a.size * a.dtype.itemsize for a in (*args, *outs))
    return pl.CostEstimate(flops=moved * 300, bytes_accessed=moved, transcendentals=0)


def settle_moments(f, first, m, v, g0, g1, m_out, v_out):
    def some(r, _):
        at = span(r * 16, 16)
        g = jnp.where(first, g0[at, :].astype(F32), g1[at, :].astype(F32))
        m_out[0, at, :], v_out[0, at, :] = moments_of(m[0, at, :], v[0, at, :], g * f)

    lax.fori_loop(0, m.shape[1] // 16, some, None)


def moment_specs(rows, cols):
    part = pl.BlockSpec((1, rows // GROUP, cols), lambda i: (i // GROUP, i % GROUP, 0))
    one = pl.BlockSpec((rows // GROUP, cols), lambda i: (jnp.minimum(i, GROUP - 1), 0))
    two = pl.BlockSpec((rows // GROUP, cols), lambda i: (jnp.maximum(i - GROUP, 0), 0))
    return part, one, two


def settle_up_kernel(factor_ref, *refs):
    ins, outs = refs[:10], refs[10:]
    for n in range(2):
        m, v, g0, g1, w = ins[5 * n : 5 * n + 5]
        m_out, v_out, w_out = outs[3 * n : 3 * n + 3]
        settle_moments(factor_ref[0:1, 0:1], pl.program_id(0) < GROUP, m, v, g0, g1, m_out, v_out)
        w_out[ALL] = w[ALL]


def settle_up(factor, *args):
    _, rows, cols = args[0].shape
    part, one, two = moment_specs(rows, cols)
    whole = pl.BlockSpec((1, rows, cols), lambda i: (i // GROUP, i % GROUP, 0))
    outs = [shape(a.shape, a.dtype) for n in range(2) for a in (args[5 * n], args[5 * n + 1], args[5 * n + 4])]
    return pl.pallas_call(
        settle_up_kernel,
        grid=(2 * GROUP,),
        in_specs=[pl.BlockSpec((8, LANES), lambda i: (0, 0))] + [part, part, one, two, whole] * 2,
        out_specs=[part, part, whole] * 2,
        out_shape=outs,
        compiler_params=params(),
        cost_estimate=cost(args, outs),
        name="settle_up",
    )(factor, *args)


def settle_down_kernel(factor_ref, m, v, g0, g1, mine, other, g_all, w_any, m_out, v_out, w_out, w_buf, stage, load, store):
    i = pl.program_id(0)
    n = stage.shape[1]
    f = factor_ref[0:1, 0:1]

    def rows(k):
        return span(lax.div(k, 2) * (EARLY + LATE) + lax.rem(k, 2) * n, n)

    def into(k):
        return local(w_any.at[1, rows(k), :], w_buf.at[lax.rem(k, 2)], load.at[lax.rem(k, 2)])

    def out(k):
        return local(stage.at[lax.rem(k, 2)], w_out.at[1, rows(k), :], store.at[lax.rem(k, 2)])

    pl.when(i == 0)(lambda: into(i).start())
    pl.when(i + 1 < pl.num_programs(0))(lambda: into(i + 1).start())
    settle_moments(f, i < GROUP, m, v, g0, g1, m_out, v_out)
    pl.when(i > 1)(lambda: out(i - 2).wait())
    into(i).wait()
    even = lax.rem(lax.axis_index("rep"), 2) == 0
    slot = lax.rem(i, 2)

    def some(r, _):
        at = span(r * 16, 16)
        one, two = mine[at, :], other[at, :]
        new = moments_of(jnp.where(even, one, two), jnp.where(even, two, one), g_all[at, :].astype(F32) * f)
        stage[slot, at, :] = weight_of(w_buf[slot, at, :].astype(F32), *new)

    lax.fori_loop(0, n // 16, some, None)
    out(i).start()

    @pl.when(i == pl.num_programs(0) - 1)
    def _():
        wait([out(i - 1), out(i)])


def settle_down(factor, m, v, g0, g1, mine, other, g_all, w):
    _, rows, cols = m.shape
    part, one, two = moment_specs(rows, cols)
    tile = EARLY // 2
    early = pl.BlockSpec((tile, cols), lambda i: (i, 0))
    outs = [shape(m.shape, F32), shape(v.shape, F32), shape(w.shape)]
    args = (m, v, g0, g1, mine, other, g_all)
    return pl.pallas_call(
        settle_down_kernel,
        grid=(2 * GROUP,),
        in_specs=[pl.BlockSpec((8, LANES), lambda i: (0, 0)), part, part, one, two, early, early, early, ANY],
        out_specs=[part, part, ANY],
        out_shape=outs,
        scratch_shapes=[VMEM((2, tile, cols), BF)] * 2 + [DMA((2,))] * 2,
        compiler_params=params(),
        cost_estimate=cost(args, outs),
        name="settle_down",
    )(factor, *args, w)


def place_kernel(own, from_left, from_right, head, tail, _, out, sem):
    me, right, left, across = around()
    block = EARLY + LATE
    half = head.shape[0]
    copies = []

    def put(src, layer, at, n):
        copies.append(local(src, out.at[layer, span(at, n), :], sem.at[len(copies)]))

    for src, owner in ((own, me), (from_left, left), (from_right, right)):
        put(src.at[pl.ds(0, block), :], 0, owner * block, block)
        put(src.at[pl.ds(block, LATE), :], 1, owner * block + EARLY, LATE)
    put(head, 0, across * block, half)
    put(tail.at[pl.ds(0, block - half), :], 0, across * block + half, block - half)
    put(tail.at[pl.ds(block - half, LATE), :], 1, across * block + EARLY, LATE)
    start(copies)
    wait(copies)


def place(blocks, out):
    return pl.pallas_call(
        place_kernel,
        in_specs=[pl.BlockSpec(memory_space=VMEM)] * len(blocks) + [ANY],
        out_specs=ANY,
        out_shape=shape(out.shape),
        scratch_shapes=[DMA((9,))],
        input_output_aliases={len(blocks): 0},
        compiler_params=params(),
        name="place",
    )(*blocks, out)


def solution(mesh):
    def step(x, dy, wg, wu, wd, mg, mu, md, vg, vu, vd):
        x, dy = x[0], dy[0]
        gate, up, at0, h, a1, at1, dyt, mine = forward(x, dy, wg, wu, wd, md, vd)
        _, _, g1, u1, d1, g0, u0, d0, other, d1_all, sq = backward(a1, at1, dy, dyt, at0, gate, up, h, wg, wu, wd, mine)
        all_g, all_u, own, factor = gather(sq, (mg, mu, md, vg, vu, vd), (wg, wu, wd), (g0, g1, u0, u1, d0, d1))
        to_right, to_left = ([(i, (i + away) % GROUP) for i in range(GROUP)] for away in (1, HOPS))
        half = own.shape[0] // 2
        from_left, from_right = lax.ppermute(own, "dp", to_right), lax.ppermute(own, "dp", to_left)
        mg, vg, new_g, mu, vu, new_u = settle_up(factor, mg, vg, g0, g1, all_g, mu, vu, u0, u1, all_u)
        from_left, from_right, new_g, factor = lax.optimization_barrier((from_left, from_right, new_g, factor))
        head, tail = lax.ppermute(from_left[:half], "dp", to_right), lax.ppermute(from_right[half:], "dp", to_left)
        md, vd, new_d = settle_down(factor, md, vd, d0, d1, mine, other, d1_all, wd)
        new_d = place((own, from_left, from_right, head, tail), new_d)
        return new_g, new_u, new_d, mg, mu, md, vg, vu, vd

    whole, part = P(), P(None, "dp", None)
    return jax.shard_map(
        step,
        mesh=mesh,
        in_specs=(P(("rep", "dp")),) * 2 + (whole,) * 3 + (part,) * 6,
        out_specs=(P("rep"),) * 3 + (P("rep", "dp", None),) * 6,
        check_vma=False,
    )
```

```python
import functools

import jax
import jax.numpy as jnp
from jax import lax
from jax.experimental import pallas as pl
from jax.experimental.pallas import tpu as pltpu
from jax.sharding import PartitionSpec as P

BF = jnp.bfloat16
F32 = jnp.float32
VMEM = pltpu.VMEM
DMA = pltpu.SemaphoreType.DMA
NN = (((1,), (0,)), ((), ()))
NT = (((1,), (1,)), ((), ()))
ONE = pl.Buffered(1)
ANY = pl.BlockSpec(memory_space=pl.ANY)
ALL = ...
LANES = 128
CHUNK = 256
STEPS = 11
LAST = STEPS - 1
TILE = 512
GROUP = 4
HOPS = GROUP - 1
EARLY = 576
LATE = 128

SUMS = (8, LANES)
FACTOR = pl.BlockSpec(SUMS, lambda i: (0, 0))


def shape(dims, dtype=BF):
    return jax.ShapeDtypeStruct(dims, dtype)


def params(collective_id=None):
    limit = 67_000_000
    if collective_id is None:
        return pltpu.CompilerParams(vmem_limit_bytes=limit)
    return pltpu.CompilerParams(vmem_limit_bytes=limit, collective_id=collective_id, has_side_effects=True)


def dot(a, b, dims):
    return lax.dot_general(a, b, dims, preferred_element_type=F32)


def span(start, size, multiple=16):
    return pl.ds(pl.multiple_of(start, multiple), size)


def local(src, dst, sem):
    return pltpu.make_async_copy(src, dst, sem)


def remote(src, dst, sent, received, to, axis="dp"):
    return pltpu.make_async_remote_copy(
        src_ref=src, dst_ref=dst, send_sem=sent, recv_sem=received, device_id={axis: to}, device_id_type=pl.DeviceIdType.MESH
    )


def around():
    me = lax.axis_index("dp")
    return (me, *(lax.rem(me + away, GROUP) for away in (1, HOPS, 2)))


def partner():
    rep = lax.axis_index("rep")
    return rep + 1 - 2 * lax.rem(rep, 2)


def greet(devices, groups=()):
    barrier = pltpu.get_barrier_semaphore()
    for axis, others in (("dp", devices), ("rep", groups)):
        for other in others:
            pl.semaphore_signal(barrier, inc=1, device_id={axis: other}, device_id_type=pl.DeviceIdType.MESH)
    pl.semaphore_wait(barrier, len(devices) + len(groups))


def start(copies):
    for c in copies:
        c.start()


def wait(copies):
    for c in copies:
        c.wait()


def first_strip(c):
    return jnp.where(c == LAST, 5, jnp.where(c % 2 == 0, c // 2, STEPS + c // 2))


def second_strip(c):
    return jnp.where(c == LAST, 16, jnp.where(c % 2 == 0, c // 2 + 6, c // 2 + 17))


def normed(wide):
    scale = lax.rsqrt(jnp.mean(wide * wide, -1, keepdims=True) + 1e-6)
    return (wide * scale).astype(BF), scale


def spread(source, dest, near_s, near_r, far_s, far_r, rows):
    me, right, left, _ = around()
    half = rows // 2
    to = (right, left)

    def near(d, n):
        part = n if d == 0 else 1 - n
        return remote(source.at[span(part * half, half), :], dest.at[span(me * rows + part * half, half), :], near_s.at[d, n], near_r.at[d, n], to[d])

    def far(d):
        spot = dest.at[span((left, right)[d] * rows + d * half, half), :]
        return remote(spot, spot, far_s.at[d], far_r.at[d], to[d])

    ways = range(2)
    return [near(d, 0) for d in ways], [near(d, 1) for d in ways], [far(d) for d in ways]


def spread_scratch():
    return [DMA((2, 2))] * 2 + [DMA((2,))] * 3


def forward_kernel(x_ref, dy_ref, wg_ref, wu_ref, wd_ref, m_ref, v_ref, gate_ref, up_ref, at0_ref, h_ref, a1_ref, at1_ref, dyt_ref, mine_ref, act, moment, *sems):
    step = pl.program_id(0)
    me, right, left, _ = around()
    kind = lax.rem(lax.axis_index("rep"), 2)
    bounce = sems[-1]
    to_stage = [local(ref.at[1, pl.ds(0, EARLY), :], moment, bounce.at[0]) for ref in (m_ref, v_ref)]
    from_stage = local(moment, mine_ref.at[span(me * EARLY, EARLY), :], bounce.at[1])
    near0, near1, far = spread(moment, mine_ref, *sems[:-1], EARLY)

    @pl.when(step == 0)
    def _():
        for n, copy in enumerate(to_stage):
            pl.when(kind == n)(copy.start)
        greet((right, left))
        to_stage[0].wait()
        start(near0 + near1 + [from_stage])

    @pl.when(step == 5)
    def _():
        from_stage.wait()
        wait(near0)
        start(far)

    dyt_ref[ALL] = dy_ref[ALL].T
    sub = TILE // 2
    for i in range(2):
        rows = slice(i * sub, (i + 1) * sub)
        a, _ = normed(x_ref[rows, :].astype(F32))
        at0_ref[:, rows] = a.T
        for c in range(STEPS):
            cols = slice(CHUNK * c, CHUNK * (c + 1))
            gate = dot(a, wg_ref[:, cols], NN)
            up = dot(a, wu_ref[:, cols], NN)
            gate_ref[rows, cols] = gate
            up_ref[rows, cols] = up
            act[rows, cols] = (gate * jax.nn.sigmoid(gate) * up).astype(BF)
    for i in range(2):
        rows = slice(i * sub, (i + 1) * sub)
        down = dot(act[rows, :], wd_ref[ALL], NN).astype(BF)
        h = (x_ref[rows, :].astype(F32) + down.astype(F32)).astype(BF)
        h_ref[rows, :] = h
        a1, _ = normed(h.astype(F32))
        a1_ref[rows, :] = a1
        at1_ref[:, rows] = a1.T

    @pl.when(step == pl.num_programs(0) - 1)
    def _():
        wait(near1 + far)


def forward(x, dy, wg, wu, wd, m, v):
    tokens, d = x.shape
    ff = wg.shape[2]
    row = pl.BlockSpec((TILE, d), lambda i: (i, 0))
    col = pl.BlockSpec((d, TILE), lambda i: (0, i))
    wide = pl.BlockSpec((TILE, ff), lambda i: (i, 0))
    up_spec = pl.BlockSpec((None, d, ff), lambda i: (0, 0, 0), pipeline_mode=ONE)
    down_spec = pl.BlockSpec((None, ff, d), lambda i: (0, 0, 0), pipeline_mode=ONE)
    across, along = shape((d, tokens)), shape((tokens, d))
    return pl.pallas_call(
        forward_kernel,
        grid=(tokens // TILE,),
        in_specs=[row, row, up_spec, up_spec, down_spec, ANY, ANY],
        out_specs=[wide, wide, col, row, row, col, col, ANY],
        out_shape=[shape((tokens, ff), F32)] * 2 + [across, along, along, across, across, shape((GROUP * EARLY, d), F32)],
        scratch_shapes=[VMEM((TILE, ff), BF), VMEM((EARLY, d), F32)] + spread_scratch(),
        compiler_params=params(4),
        name="fwd0",
    )(x, dy, wg, wu, wd, m, v)


class Ring:
    def __init__(self, item, rows, refs, emit):
        self.item = item
        self.rows = rows
        self.term, self.recv, self.send, self.fin, self.ssem, self.rsem, self.total = refs
        self.emit = emit

    def mine(self, h, d, k, half, away):
        me = lax.axis_index("dp")
        away = away + h
        block = lax.rem(me + 2 * GROUP - away, GROUP) if d == 0 else lax.rem(me + away, GROUP)
        return lax.rem(k, self.term.shape[0]), span(block * 2 * half + d * half, half, half), slice(None)

    def copy(self, h, d, k, half):
        _, right, left, _ = around()
        spot = (d, lax.rem(k, 2), pl.ds(0, half), slice(None))
        src = self.term.at[self.mine(h, d, k, half, 1)] if h == 0 else self.send.at[h - 1, *spot]
        sems = self.ssem.at[h, *spot[:2]], self.rsem.at[h, *spot[:2]]
        return remote(src, self.recv.at[h, *spot], *sems, (right, left)[d])

    def each(self, t, body):
        there, k = self.item(t)
        for condition, half in self.rows:
            where = there if condition is None else jnp.logical_and(there, condition(k))
            pl.when(where)(functools.partial(body, k, half))

    def point(self, t):
        ways = range(2)

        def arrived(h, k, half):
            wait([self.copy(h, d, k, half) for d in ways])

        def add(h, k, half):
            slot = lax.rem(k, 2)
            for d in ways:
                spot = (d, slot, pl.ds(0, half), slice(None))
                value = (self.recv[h, *spot].astype(F32) + self.term[self.mine(h, d, k, half, 2)].astype(F32)).astype(BF)
                if h < HOPS - 1:
                    self.send[h, *spot] = value
                else:
                    self.fin[slot, pl.ds(d * half, half), :] = value
                    square = value.astype(F32) ** 2
                    parts = [square[:, LANES * i : LANES * (i + 1)] for i in range(square.shape[1] // LANES)]
                    self.total[ALL] += jnp.sum(functools.reduce(jnp.add, parts).reshape(half // 8, 8, LANES), 0)

        def leave(h, k, half):
            start([self.copy(h, d, k, half) for d in ways])

        def out(k, half):
            start(self.emit(k, lax.rem(k, 2), 2 * half))

        def gone(k, half):
            wait(self.emit(k, lax.rem(k, 2), 2 * half))

        for h in range(HOPS):
            self.each(t - 1 - h, functools.partial(arrived, h))
        self.each(t - HOPS - 1, gone)
        for h in range(HOPS):
            self.each(t - 1 - h, functools.partial(add, h))
        for h in range(HOPS):
            self.each(t - h, functools.partial(leave, h))
        self.each(t - HOPS, out)


def rings(refs, g_out, u_out, d_out):
    (g_term, u_term, d_term, g_recv, u_recv, d_recv, g_send, u_send, d_send, g_fin, u_fin, d_fin, ssem, rsem, fsem, total) = refs
    me = lax.axis_index("dp")

    def every(t):
        return jnp.logical_and(t >= 0, t < STEPS), t

    def pairs(t):
        last = t == STEPS
        return jnp.logical_or(last, jnp.logical_and(jnp.logical_and(t >= 2, t < STEPS), lax.rem(t, 2) == 0)), jnp.where(last, 5, lax.div(t, 2) - 1)

    def columns(fin, out, sem):
        def emit(k, slot, rows):
            return [
                local(fin.at[slot, :, pl.ds(LANES * i, LANES)], out.at[:, span(LANES * strip(k), LANES, LANES)], sem.at[slot, i])
                for i, strip in enumerate((first_strip, second_strip))
            ]

        return emit

    def down(k, slot, rows):
        odd = lax.rem(me, 2)
        at = LANES * k + 64 * odd if rows == LANES else 640 * (1 - odd)
        return [local(d_fin.at[slot, pl.ds(0, rows), :], d_out.at[span(at, rows, 64), :], fsem.at[2, slot, 0])]

    halves = [(None, LANES)]
    return (
        Ring(every, halves, (g_term, g_recv, g_send, g_fin, ssem.at[0], rsem.at[0], total), columns(g_fin, g_out, fsem.at[0])),
        Ring(every, halves, (u_term, u_recv, u_send, u_fin, ssem.at[1], rsem.at[1], total), columns(u_fin, u_out, fsem.at[1])),
        Ring(pairs, [(lambda k: k < 5, 64), (lambda k: k == 5, 32)], (d_term, d_recv, d_send, d_fin, ssem.at[2], rsem.at[2], total), down),
    )


def ring_scratch(d):
    up, down = (2, 2, LANES, CHUNK), (2, 2, 64, d)
    return (
        [VMEM((GROUP, d, CHUNK), BF)] * 2
        + [VMEM((3, TILE, d), BF)]
        + [VMEM((HOPS, *up), BF)] * 2
        + [VMEM((HOPS, *down), BF)]
        + [VMEM((HOPS - 1, *up), BF)] * 2
        + [VMEM((HOPS - 1, *down), BF)]
        + [VMEM((2, CHUNK, CHUNK), BF)] * 2
        + [VMEM((2, LANES, d), BF), DMA((3, HOPS, 2, 2)), DMA((3, HOPS, 2, 2)), DMA((3, 2, 2)), VMEM(SUMS, F32)]
    )


def weight_gradients(c, at_ref, dyt_ref, dg, du, act, refs, g, u):
    half = at_ref.shape[0] // 2
    halves = [slice(0, half), slice(half, 2 * half)]
    for term, right in zip(refs[:2], (dg, du)):
        for rows in halves:
            term[lax.rem(c, GROUP), rows, :] = dot(at_ref[rows, :], right[ALL], NN).astype(BF)
    g.point(c)
    for rows in halves:
        value = dot(dyt_ref[rows, :], act[ALL], NN).astype(BF).T
        refs[2][lax.rem(c // 2, 3), span(CHUNK * lax.rem(c, 2), CHUNK), rows] = value
    u.point(c)


def gated(gate, up, dact):
    s = jax.nn.sigmoid(gate)
    silu = gate * s
    return (silu * up).astype(BF), (dact * silu).astype(BF), (dact * up * (s + silu * (1.0 - s))).astype(BF)


def strips(c):
    return first_strip(c), second_strip(c)


def columns_in(src, dst, sem, c):
    return [local(src.at[:, span(LANES * k, LANES, LANES)], dst.at[:, pl.ds(LANES * i, LANES)], sem.at[i]) for i, k in enumerate(strips(c))]


def rows_in(src, dst, sem, c):
    return [local(src.at[span(LANES * k, LANES), :], dst.at[pl.ds(LANES * i, LANES), :], sem.at[i]) for i, k in enumerate(strips(c))]


def backward_kernel(a_any, at1_any, dy_any, dyt_any, at0_any, gate_any, up_any, h_any, wg_any, wu_any, wd_any, mine_ref, dgate_out, dup_out, g1, u1, d1, g0, u0, d0, other_ref, early_ref, sq_ref, own, osem, msem, wsem, *scratch):
    refs, sems = scratch[:16], scratch[16:]
    me, right, left, _ = around()
    tokens, width = a_any.shape
    tiles = tokens // TILE
    exchange = remote(mine_ref, other_ref, msem.at[0], msem.at[1], partner(), "rep")
    bounce = sems[-1]
    to_stage = local(d1.at[pl.ds(0, EARLY), :], own, bounce.at[0])
    from_stage = local(own, early_ref.at[span(me * EARLY, EARLY), :], bounce.at[1])
    near0, near1, far = spread(own, early_ref, *sems[:-1], EARLY)

    def layer1(a_ref, at_ref, dy_ref, dyt_ref, act, dg, du, wg, wu, wd, tile_sem, whole_sem):
        g, u, d = rings(refs, g1, u1, d1)

        def weights(c):
            slot = lax.rem(c, 2)
            return (
                columns_in(wg_any.at[1], wg.at[slot], wsem.at[0, slot], c)
                + columns_in(wu_any.at[1], wu.at[slot], wsem.at[1, slot], c)
                + rows_in(wd_any.at[1], wd.at[slot], wsem.at[2, slot], c)
            )

        def arrive(i):
            rows = span(TILE * i, TILE)
            return [local(src.at[rows, :], dst.at[rows, :], tile_sem.at[n, i]) for n, (src, dst) in enumerate(((a_any, a_ref), (dy_any, dy_ref)))]

        whole = [local(at1_any, at_ref, whole_sem.at[0]), local(dyt_any, dyt_ref, whole_sem.at[1])]

        def put(k):
            cols = span(CHUNK * k, CHUNK, CHUNK)
            return [local(dg, dgate_out.at[:, cols], osem.at[0]), local(du, dup_out.at[:, cols], osem.at[1])]

        start(weights(jnp.int32(0)))
        for i in range(tiles):
            start(arrive(i))
        start(whole)
        refs[-1][ALL] = jnp.zeros_like(refs[-1])
        greet((right, left), (partner(),))

        def chunk(c, _):
            slot = lax.rem(c, 2)
            pl.when(c < LAST)(lambda: start(weights(c + 1)))
            pl.when(c > 0)(lambda: wait(put(c - 1)))
            pl.when(c == 2)(exchange.start)
            wait(weights(c))

            def some(rows):
                gate = dot(a_ref[rows, :], wg[slot], NN)
                up = dot(a_ref[rows, :], wu[slot], NN)
                dact = dot(dy_ref[rows, :], wd[slot], NT).astype(BF).astype(F32)
                act[rows, :], du[rows, :], dg[rows, :] = gated(gate, up, dact)

            @pl.when(c == 0)
            def _():
                def one(i, _):
                    wait(arrive(i))
                    some(span(TILE * i, TILE))

                lax.fori_loop(0, tiles, one, None)
                wait(whole)

            @pl.when(c > 0)
            def _():
                for i in range(tiles):
                    some(slice(TILE * i, TILE * (i + 1)))

            d.point(c)
            start(put(c))
            weight_gradients(c, at_ref, dyt_ref, dg, du, act, refs, g, u)

        lax.fori_loop(0, STEPS, chunk, None)
        wait(put(LAST))

    def input_gradient(dh_ref, dht_ref, wg, wu, dg_buf, du_buf, h_buf, dy_buf, sem, tile_sem):
        g, u, d = rings(refs, g1, u1, d1)
        n = dg_buf.shape[1]

        def tile(j):
            slot = lax.rem(j, 2)
            rows = span(n * j, n)
            pairs = ((dgate_out, dg_buf), (dup_out, du_buf), (h_any, h_buf), (dy_any, dy_buf))
            return [local(src.at[rows, :], dst.at[slot], tile_sem.at[i, slot]) for i, (src, dst) in enumerate(pairs)]

        start(tile(jnp.int32(0)))
        copies = [columns_in(src.at[1], dst.at[:, pl.ds(CHUNK * c, CHUNK)], sem.at[i, c], jnp.int32(c)) for i, (src, dst) in enumerate(((wg_any, wg), (wu_any, wu))) for c in range(STEPS)]
        start(sum(copies, []))
        wait(sum(copies, []))

        def one(j, _):
            slot = lax.rem(j, 2)
            pl.when(j + 1 < tokens // n)(lambda: start(tile(j + 1)))

            @pl.when(jnp.logical_and(j > 0, j < HOPS + 3))
            def _():
                for ring in (d, g, u):
                    ring.point(j + LAST)

            @pl.when(j == HOPS + 2)
            def _():
                to_stage.start()
                to_stage.wait()
                start([*near0, *near1, from_stage])

            @pl.when(j == 10)
            def _():
                from_stage.wait()
                wait(near0)
                start(far)

            wait(tile(j))
            da = dot(dg_buf[slot], wg[ALL], NT).astype(BF).astype(F32) + dot(du_buf[slot], wu[ALL], NT).astype(BF).astype(F32)
            da = da.astype(BF).astype(F32)
            wide = h_buf[slot].astype(F32)
            _, scale = normed(wide)
            along = jnp.sum(da * wide, -1, keepdims=True) * (scale * scale * scale) / width
            back = (da * scale - wide * along).astype(BF)
            dh = (dy_buf[slot].astype(F32) + back.astype(F32)).astype(BF)
            rows = span(n * j, n, n)
            dh_ref[rows, :] = dh
            dht_ref[:, rows] = dh.T

        lax.fori_loop(0, tokens // n, one, None)

    def layer0(dh_ref, dht_ref, at_ref, gate_buf, up_buf, act, dg, du, wd, tile_sem):
        g, u, d = rings(refs, g0, u0, d0)

        def weights(c):
            slot = lax.rem(c, 2)
            return rows_in(wd_any.at[0], wd.at[slot], wsem.at[2, slot], c)

        def arrive(c, i):
            slot = lax.rem(c, 2)
            rows = span(TILE * i, TILE)
            return [copy for n, (src, dst) in enumerate(((gate_any, gate_buf), (up_any, up_buf))) for copy in columns_in(src.at[rows, :], dst.at[slot, rows, :], tile_sem.at[slot, i, n], c)]

        def fetch(c):
            start(weights(c))
            lax.fori_loop(0, tiles, lambda i, _: start(arrive(c, i)), None)

        fetch(jnp.int32(0))

        def chunk(c, _):
            slot = lax.rem(c, 2)
            pl.when(c < LAST)(lambda: fetch(c + 1))
            wait(weights(c))

            def some(i, _):
                rows = span(TILE * i, TILE)
                wait(arrive(c, i))
                dact = dot(dh_ref[rows, :], wd[slot], NT).astype(BF).astype(F32)
                act[rows, :], du[rows, :], dg[rows, :] = gated(gate_buf[slot, rows, :], up_buf[slot, rows, :], dact)

            lax.fori_loop(0, tiles, some, None)
            d.point(c)
            weight_gradients(c, at_ref, dht_ref, dg, du, act, refs, g, u)

        lax.fori_loop(0, STEPS, chunk, None)

        def drain(t, _):
            for ring in (d, g, u):
                ring.point(t)

        lax.fori_loop(STEPS, STEPS + HOPS + 2, drain, None)

    along, across = VMEM((tokens, width), BF), VMEM((width, tokens), BF)
    parts = [VMEM((tokens, CHUNK), BF)] * 3
    up_strip, down_strip = VMEM((2, width, CHUNK), BF), VMEM((2, CHUNK, width), BF)
    pl.run_scoped(layer1, along, across, along, across, *parts, up_strip, up_strip, down_strip, DMA((2, tiles)), DMA((2,)))

    def rest(dh_ref, dht_ref, at_ref, at_sem):
        ff = dgate_out.shape[1]
        fetched = local(at0_any, at_ref, at_sem.at[0])
        fetched.start()
        n = TILE // 2
        whole, wide, narrow = VMEM((width, ff), BF), VMEM((2, n, ff), BF), VMEM((2, n, width), BF)
        pl.run_scoped(functools.partial(input_gradient, dh_ref, dht_ref), whole, whole, wide, wide, narrow, narrow, DMA((2, STEPS, 2)), DMA((4, 2)))
        fetched.wait()
        strip = VMEM((2, tokens, CHUNK), F32)
        pl.run_scoped(functools.partial(layer0, dh_ref, dht_ref, at_ref), strip, strip, *parts, down_strip, DMA((2, tiles, 2, 2)))

    pl.run_scoped(rest, along, across, across, DMA((1,)))
    wait([exchange, *near1, *far])
    sq_ref[ALL] = refs[-1][ALL]


def backward(a1, at1, dy, dyt, at0, gate, up, h, wg, wu, wd, mine):
    tokens, d = a1.shape
    ff = wg.shape[2]
    wide, block_up, block_down = shape((tokens, ff)), shape((d // GROUP, ff)), shape((ff // GROUP, d))
    return pl.pallas_call(
        backward_kernel,
        in_specs=[ANY] * 12,
        out_specs=[ANY] * 10 + [pl.BlockSpec(memory_space=VMEM)],
        out_shape=[wide, wide] + [block_up, block_up, block_down] * 2 + [shape(mine.shape, F32), shape(mine.shape), shape(SUMS, F32)],
        scratch_shapes=[VMEM((EARLY, d), BF), DMA((2,)), DMA((2,)), DMA((3, 2, 2))] + ring_scratch(d) + spread_scratch(),
        compiler_params=params(1),
        name="backward",
    )(a1, at1, dy, dyt, at0, gate, up, h, wg, wu, wd, mine)


def moments_of(m, v, g):
    return 0.9 * m + 0.1 * g, 0.95 * v + 0.05 * g * g


def weight_of(w, m, v):
    return (w - 0.02 * (m * lax.rsqrt(v + 1e-8) + 0.1 * w)).astype(BF)


def gather_kernel(count, sq, mg, vg, mu, vu, md, vd, wg, wu, wd, g0, g1, u0, u1, d0, d1, wg_all, wu_all, own_a, own_b, factor_ref, *scratch):
    (stage_g, stage_u, stage_d, m_up, v_up, w_up, g_up, m_dn, v_dn, w_dn, g_dn, sums, total, load, keep_sem, near_s, near_r, far_s, far_r, sum_s, sum_r, sum_l) = scratch
    me, right, left, across = around()
    pieces, rows = stage_g.shape[0], stage_g.shape[1]
    per = pieces // 2
    block = per * rows

    for other in (right, left, across):
        pl.semaphore_signal(pltpu.get_barrier_semaphore(), inc=1, device_id={"dp": other}, device_id_type=pl.DeviceIdType.MESH)
    pl.semaphore_wait(pltpu.get_barrier_semaphore(), HOPS)
    shares = [remote(sq, sums.at[j + 1], sum_s.at[j], sum_r.at[j], lax.rem(me + j + 1, GROUP)) for j in range(HOPS)]
    shares.append(local(sq, sums.at[0], sum_l.at[0]))
    start(shares)

    def loads(i, slot, arrays, gradient, bufs, layer, row, n, base):
        m, v, w = arrays
        here = span(row, n)
        sources = (m.at[layer, here, :], v.at[layer, here, :], w.at[layer, span(base + row, n), :], gradient.at[here, :])
        return [local(s, b.at[slot, pl.ds(0, n), :], load.at[j, slot]) for j, (s, b) in enumerate(zip(sources, bufs))]

    def update(slot, bufs, stage, i, n):
        m_buf, v_buf, w_buf, g_buf = bufs
        f = total[0:1, 0:1]

        def some(r, _):
            at = span(r * 16, 16)
            m, v = moments_of(m_buf[slot, at, :], v_buf[slot, at, :], g_buf[slot, at, :].astype(F32) * f)
            stage[i, at, :] = weight_of(w_buf[slot, at, :].astype(F32), m, v)

        lax.fori_loop(0, n // 16, some, None)

    def spot(dest, i, owner, at, n):
        return dest.at[lax.div(i, per), span(owner * block + lax.rem(i, per) * rows + at, n), :]

    def near(which, dest, stage, i, d):
        sems = near_s.at[which, i, d], near_r.at[which, i, d]
        return remote(stage.at[i], spot(dest, i, me, 0, rows), *sems, (right, left)[d])

    def far(which, dest, i, d):
        place = spot(dest, i, (left, right)[d], d * (rows // 2), rows // 2)
        return remote(place, place, far_s.at[which, i, d], far_r.at[which, i, d], (right, left)[d])

    def keep(which, dest, stage, i):
        return local(stage.at[i], spot(dest, i, me, 0, rows), keep_sem.at[which, i])

    up_bufs, down_bufs = (m_up, v_up, w_up, g_up), (m_dn, v_dn, w_dn, g_dn)
    ups = ((wg_all, stage_g, (mg, vg, wg), (g0, g1)), (wu_all, stage_u, (mu, vu, wu), (u0, u1)))

    def fetch(i, arrays, gradients):
        layer = lax.div(i, per)
        for n, gradient in enumerate(gradients):

            @pl.when(layer == n)
            def _():
                start(loads(i, lax.rem(i, 2), arrays, gradient, up_bufs, layer, lax.rem(i, per) * rows, rows, me * block))

    for which, (dest, stage, arrays, gradients) in enumerate(ups):
        fetch(jnp.int32(0), arrays, gradients)
        if which == 0:
            wait(shares)
            parts = [sums[lax.rem(me + GROUP - b, GROUP)] for b in range(GROUP)]
            squares = jnp.sum(functools.reduce(jnp.add, parts), keepdims=True)
            factor = jnp.minimum(1.0, 0.5 * lax.rsqrt(squares / count + 1e-30))
            total[ALL] = jnp.broadcast_to(factor, total.shape)
            factor_ref[ALL] = jnp.broadcast_to(factor, total.shape)

        def body(i, _):
            slot = lax.rem(i, 2)

            @pl.when(i + 1 < pieces)
            def _():
                fetch(i + 1, arrays, gradients)

            wait(loads(i, slot, arrays, gradients[0], up_bufs, lax.div(i, per), lax.rem(i, per) * rows, rows, me * block))
            update(slot, up_bufs, stage, i, rows)
            start([keep(which, dest, stage, i), near(which, dest, stage, i, 0), near(which, dest, stage, i, 1)])

        lax.fori_loop(0, pieces, body, None)

    half = stage_d.shape[1]
    downs = [loads(0, n, (md, vd, wd), d0, down_bufs, 0, n * half, half, me * 2 * half) for n in range(2)]
    late = loads(0, 0, (md, vd, wd), d1, down_bufs, 1, EARLY, LATE, me * 2 * half)
    cut = own_a.shape[0] - half
    outs = [
        local(stage_d.at[0], own_a.at[pl.ds(0, half), :], sum_l.at[0]),
        local(stage_d.at[1, pl.ds(0, cut), :], own_a.at[pl.ds(half, cut), :], sum_l.at[1]),
        local(stage_d.at[1, pl.ds(cut, half - cut), :], own_b.at[pl.ds(0, half - cut), :], load.at[1, 1]),
        local(stage_d.at[2, pl.ds(0, LATE), :], own_b.at[pl.ds(half - cut, LATE), :], load.at[0, 1]),
    ]
    for copies in downs:
        start(copies)
    for n in range(2):
        wait(downs[n])
        update(n, down_bufs, stage_d, n, half)
    start(late)
    wait(late)
    update(0, down_bufs, stage_d, 2, LATE)
    start(outs)

    for which, (dest, stage, _, _) in enumerate(ups):

        def onward(i, _):
            for d in range(2):
                near(which, dest, stage, i, d).wait()
                far(which, dest, i, d).start()

        lax.fori_loop(0, pieces, onward, None)
    for which, (dest, stage, _, _) in enumerate(ups):

        def finish(i, _):
            wait([keep(which, dest, stage, i), far(which, dest, i, 0), far(which, dest, i, 1)])

        lax.fori_loop(0, pieces, finish, None)
    wait(outs)


def gather(sq, moments, weights, gradients):
    mg, mu, md, vg, vu, vd = moments
    wg, wu, wd = weights
    _, d, ff = wg.shape
    pieces, rows, half = 2 * GROUP, d // GROUP // GROUP, ff // GROUP // 2
    up, down, each = (2, rows, ff), (2, half, d), (2, pieces, 2)
    return pl.pallas_call(
        functools.partial(gather_kernel, float(wg.size + wu.size + wd.size)),
        in_specs=[ANY] * 16,
        out_specs=[ANY] * 4 + [pl.BlockSpec(memory_space=VMEM)],
        out_shape=[shape(wg.shape), shape(wu.shape)] + [shape((half + LATE // 2, d))] * 2 + [shape(SUMS, F32)],
        scratch_shapes=[VMEM((pieces, rows, ff), BF)] * 2
        + [VMEM((3, half, d), BF)]
        + [VMEM(up, F32), VMEM(up, F32), VMEM(up, BF), VMEM(up, BF)]
        + [VMEM(down, F32), VMEM(down, F32), VMEM(down, BF), VMEM(down, BF)]
        + [VMEM((GROUP, 8, LANES), F32), VMEM(SUMS, F32), DMA((4, 2)), DMA((2, pieces))]
        + [DMA(each)] * 4
        + [DMA((HOPS,)), DMA((HOPS,)), DMA((2,))],
        compiler_params=params(3),
        name="gather",
    )(sq, mg, vg, mu, vu, md, vd, wg, wu, wd, *gradients)


def cost(args, outs):
    moved = sum(a.size * a.dtype.itemsize for a in (*args, *outs))
    return pl.CostEstimate(flops=moved * 300, bytes_accessed=moved, transcendentals=0)


def settle_moments(f, first, m, v, g0, g1, m_out, v_out):
    def some(r, _):
        at = span(r * 16, 16)
        g = jnp.where(first, g0[at, :].astype(F32), g1[at, :].astype(F32))
        m_out[0, at, :], v_out[0, at, :] = moments_of(m[0, at, :], v[0, at, :], g * f)

    lax.fori_loop(0, m.shape[1] // 16, some, None)


def moment_specs(rows, cols):
    part = pl.BlockSpec((1, rows // GROUP, cols), lambda i: (i // GROUP, i % GROUP, 0))
    one = pl.BlockSpec((rows // GROUP, cols), lambda i: (jnp.minimum(i, GROUP - 1), 0))
    two = pl.BlockSpec((rows // GROUP, cols), lambda i: (jnp.maximum(i - GROUP, 0), 0))
    return part, one, two


def settle_kernel(factor_ref, *refs):
    ins, outs = refs[:14], refs[14:]
    for n in range(3):
        m, v, g0, g1 = ins[5 * n : 5 * n + 4]
        m_out, v_out = outs[3 * n : 3 * n + 2]
        settle_moments(factor_ref[0:1, 0:1], pl.program_id(0) < GROUP, m, v, g0, g1, m_out, v_out)
        if n < 2:
            outs[3 * n + 2][ALL] = ins[5 * n + 4][ALL]


def settle(factor, *args):
    in_specs, out_specs, outs = [FACTOR], [], []
    for n in range(3):
        some = args[5 * n : 5 * n + 5]
        _, rows, cols = some[0].shape
        part, one, two = moment_specs(rows, cols)
        whole = [pl.BlockSpec((1, rows, cols), lambda i: (i // GROUP, i % GROUP, 0))] * (n < 2)
        in_specs += [part, part, one, two, *whole]
        out_specs += [part, part, *whole]
        outs += [shape(a.shape, a.dtype) for a in (*some[:2], *some[4:])]
    return pl.pallas_call(
        settle_kernel,
        grid=(2 * GROUP,),
        in_specs=in_specs,
        out_specs=out_specs,
        out_shape=outs,
        compiler_params=params(),
        cost_estimate=cost(args, outs),
        name="settle",
    )(factor, *args)


def placed(a, b, out, owner, sems):
    block = EARLY + LATE
    half = a.shape[0]
    return [
        local(a, out.at[0, span(owner * block, half), :], sems.at[0]),
        local(b.at[pl.ds(0, block - half), :], out.at[0, span(owner * block + half, block - half), :], sems.at[1]),
        local(b.at[pl.ds(block - half, LATE), :], out.at[1, span(owner * block + EARLY, LATE), :], sems.at[2]),
    ]


def early_kernel(factor_ref, mine, other, g_all, own_a, own_b, left_a, left_b, right_a, right_b, w_any, w_out, w_buf, stage, load, store, put):
    i = pl.program_id(0)
    n = stage.shape[1]
    f = factor_ref[0:1, 0:1]
    me, right, left, _ = around()
    blocks = placed(own_a, own_b, w_out, me, put.at[0]) + placed(left_a, left_b, w_out, left, put.at[1]) + placed(right_a, right_b, w_out, right, put.at[2])

    def rows(k):
        return span(lax.div(k, 2) * (EARLY + LATE) + lax.rem(k, 2) * n, n)

    def into(k):
        return local(w_any.at[1, rows(k), :], w_buf.at[lax.rem(k, 2)], load.at[lax.rem(k, 2)])

    def out(k):
        return local(stage.at[lax.rem(k, 2)], w_out.at[1, rows(k), :], store.at[lax.rem(k, 2)])

    pl.when(i == 0)(lambda: start([into(i), *blocks]))
    pl.when(i + 1 < pl.num_programs(0))(lambda: into(i + 1).start())
    pl.when(i > 1)(lambda: out(i - 2).wait())
    into(i).wait()
    even = lax.rem(lax.axis_index("rep"), 2) == 0
    slot = lax.rem(i, 2)

    def some(r, _):
        at = span(r * 16, 16)
        one, two = mine[at, :], other[at, :]
        new = moments_of(jnp.where(even, one, two), jnp.where(even, two, one), g_all[at, :].astype(F32) * f)
        stage[slot, at, :] = weight_of(w_buf[slot, at, :].astype(F32), *new)

    lax.fori_loop(0, n // 16, some, None)
    out(i).start()

    @pl.when(i == pl.num_programs(0) - 1)
    def _():
        wait([out(i - 1), out(i), *blocks])


def early(factor, mine, other, g_all, blocks, w):
    tile, cols = EARLY // 2, w.shape[2]
    part = pl.BlockSpec((tile, cols), lambda i: (i, 0))
    whole = pl.BlockSpec(blocks[0].shape, lambda i: (0, 0), pipeline_mode=ONE)
    outs = shape(w.shape)
    return pl.pallas_call(
        early_kernel,
        grid=(2 * GROUP,),
        in_specs=[FACTOR, part, part, part] + [whole] * 6 + [ANY],
        out_specs=ANY,
        out_shape=outs,
        scratch_shapes=[VMEM((2, tile, cols), BF)] * 2 + [DMA((2,))] * 2 + [DMA((3, 3))],
        compiler_params=params(),
        cost_estimate=cost((mine, other, g_all, *blocks), (outs,)),
        name="early",
    )(factor, mine, other, g_all, *blocks, w)


def place_kernel(a, b, _, out, sem):
    copies = placed(a, b, out, around()[-1], sem)
    start(copies)
    wait(copies)


def place(a, b, out):
    return pl.pallas_call(
        place_kernel,
        in_specs=[pl.BlockSpec(memory_space=VMEM)] * 2 + [ANY],
        out_specs=ANY,
        out_shape=shape(out.shape),
        scratch_shapes=[DMA((3,))],
        input_output_aliases={2: 0},
        compiler_params=params(),
        name="place",
    )(a, b, out)


def solution(mesh):
    def step(x, dy, wg, wu, wd, mg, mu, md, vg, vu, vd):
        x, dy = x[0], dy[0]
        gate, up, at0, h, a1, at1, dyt, mine = forward(x, dy, wg, wu, wd, md, vd)
        _, _, g1, u1, d1, g0, u0, d0, other, d1_all, sq = backward(a1, at1, dy, dyt, at0, gate, up, h, wg, wu, wd, mine)
        all_g, all_u, *own, factor = gather(sq, (mg, mu, md, vg, vu, vd), (wg, wu, wd), (g0, g1, u0, u1, d0, d1))
        to_right, to_left = ([(i, (i + away) % GROUP) for i in range(GROUP)] for away in (1, HOPS))
        from_left = [lax.ppermute(half, "dp", to_right) for half in own]
        from_right = [lax.ppermute(half, "dp", to_left) for half in own]
        mg, vg, new_g, mu, vu, new_u, md, vd = settle(factor, mg, vg, g0, g1, all_g, mu, vu, u0, u1, all_u, md, vd, d0, d1)
        from_left, from_right, new_g, factor = lax.optimization_barrier((from_left, from_right, new_g, factor))
        head, tail = lax.ppermute(from_left[0], "dp", to_right), lax.ppermute(from_right[1], "dp", to_left)
        new_d = early(factor, mine, other, d1_all, (*own, *from_left, *from_right), wd)
        new_d = place(head, tail, new_d)
        return new_g, new_u, new_d, mg, mu, md, vg, vu, vd

    whole, part = P(), P(None, "dp", None)
    return jax.shard_map(
        step,
        mesh=mesh,
        in_specs=(P(("rep", "dp")),) * 2 + (whole,) * 3 + (part,) * 6,
        out_specs=(P("rep"),) * 3 + (P("rep", "dp", None),) * 6,
        check_vma=False,
    )
```
